32 devices in a mesh: coil: 8 (over y, x, core), kz: 4 (over z).
Axes of the slice: x: 2, y: 2, z: 4, core: 2. Of those that a mesh axis runs over, the one named last changes fastest.
Arguments:
- kdata: bfloat16 [2, 64, 8, 256, 512], P(None, 'kz', 'coil'), may hold values from -6 to 6
- spoke_angle: int32 [256], replicated, may hold values from 0 to 63
- spoke_count: int32 [64], P('kz'), may hold values from 128 to 256
- block_index: int32 [64, 4], replicated, may hold values from 0 to 511
- interp: bfloat16 [64, 4, 128, 128], replicated, may hold values from -0.5 to 0.5
- sens_maps: bfloat16 [2, 8, 256, 256], P(None, 'coil'), may hold values from -5 to 5
Outputs:
- image: float32 [2, 64, 256, 256], P(None, 'kz', 'coil')
The draws below stay inside these ranges and needn't reach their ends.
Inputs may be any that keep to these rules, and one draw needn't show every extreme that they name: Partition p uses its first spoke_count[p] spokes. `block_index`: several segments may hit the same grid block.
All inputs are finite; a program needn't handle non-finite values.
Results may differ from the reference program's by a relative error of at most 0.0059.
Values sent between devices are 32-bit elements; how exact they have to be, the bound alone decides.
A program may use at most 128 MiB of HBM per device.

```python
import jax
import jax.numpy as jnp
from jax import lax

N = 256
SAMPLES = 512
SEG_LEN = 128
SEGS = 4
BLOCKS = 512
SPOKES = 256
ANGLES = 64
KZ = 64
COILS = 8


def place_ends(values, key, smallest, largest):
    spot = [jax.random.randint(jax.random.fold_in(key, axis), (), 0, length) for axis, length in enumerate(values.shape)]
    main_axis = values.shape.index(max(values.shape))
    next_to = spot[:main_axis] + [(spot[main_axis] + 1) % values.shape[main_axis]] + spot[main_axis + 1:]
    return values.at[tuple(spot)].set(smallest).at[tuple(next_to)].set(largest)


def level_of(stream_key, dims, cuts, smallest, largest):
    def one(dim, blocks):
        steps = jax.random.uniform(jax.random.fold_in(jax.random.fold_in(stream_key, 6), dim), (blocks,), jnp.float32, smallest / len(cuts), largest / len(cuts))
        return jnp.repeat(jnp.exp(steps), dims[dim] // blocks).reshape((-1,) + (1,) * (len(dims) - dim - 1))

    factor_of = one(*cuts[0])
    for cut in cuts[1:]:
        factor_of = factor_of * one(*cut)
    return factor_of


def centred(rng, shape, width, limit, cuts=(), kind=jnp.bfloat16):
    values = width * jax.random.normal(rng, shape, jnp.float32)
    if cuts:
        values = values * level_of(rng, shape, cuts, -0.22, 0.18)
    return jnp.clip(values, -limit, limit).astype(kind)


def setup_inputs(seed: int = 0) -> dict:
    arg_keys = jax.random.split(jax.random.key(seed), 7)
    return {
        "kdata": centred(arg_keys[0], (2, KZ, COILS, SPOKES, SAMPLES), 1.0, 6.0, ((1, 4), (2, 8))),
        "spoke_angle": place_ends(jax.random.randint(arg_keys[1], (SPOKES,), 0, ANGLES), jax.random.fold_in(arg_keys[1], 1), 0, ANGLES - 1).astype(jnp.int32),
        "spoke_count": place_ends(jax.random.randint(arg_keys[2], (KZ,), SPOKES // 2, SPOKES + 1), jax.random.fold_in(arg_keys[2], 1), SPOKES // 2, SPOKES).astype(jnp.int32),
        "block_index": place_ends(jax.random.randint(arg_keys[3], (ANGLES, SEGS), 0, BLOCKS), jax.random.fold_in(arg_keys[3], 1), 0, BLOCKS - 1).astype(jnp.int32),
        "interp": centred(arg_keys[4], (ANGLES, SEGS, SEG_LEN, SEG_LEN), SEG_LEN ** -0.5, 0.5),
        "sens_maps": centred(arg_keys[5], (2, COILS, N, N), (COILS ** -0.5), 5.0, ((1, 8),)),
    }


def dft_tables(length, dtype):
    index = jnp.arange(length, dtype=jnp.int32)
    product = index[:, None] * index[None, :] % length
    phase = product.astype(jnp.float32) * (2.0 * jnp.pi / length)
    scale = 1.0 / jnp.sqrt(jnp.float32(length))
    return ((jnp.cos(phase) * scale).astype(dtype), (jnp.sin(phase) * scale).astype(dtype))

def spoke_weights(spoke_count, spoke_angle, angles, spokes):
    position = jnp.arange(spokes, dtype=jnp.int32)
    used = position[None, :] < spoke_count[:, None]
    match = spoke_angle[:, None] == jnp.arange(angles, dtype=jnp.int32)[None, :]
    return (used[:, :, None] & match[None, :, :]).astype(jnp.bfloat16)

def coil_image(data, weights, interp, block_index, cos_t, sin_t):
    f32 = jnp.float32
    binned = jnp.einsum('rpsn,psa->rpan', data.astype(f32), weights.astype(f32)).astype(jnp.bfloat16)
    rdim, pdim, adim, mdim = binned.shape
    seg = interp.shape[2]
    gdim = mdim // seg
    side = cos_t.shape[0]
    pieces = binned.reshape(rdim, pdim, adim, gdim, seg)
    contrib = jnp.einsum('rpagj,agjt->rpagt', pieces.astype(f32), interp.astype(f32))
    flat = jnp.zeros((rdim, pdim, side * side // seg, seg), f32)
    flat = flat.at[:, :, block_index.reshape(-1)].add(contrib.reshape(rdim, pdim, adim * gdim, seg))
    grid = flat.reshape(rdim, pdim, side, side).astype(jnp.bfloat16)
    cosf = cos_t.astype(f32)
    sinf = sin_t.astype(f32)
    grid_re = grid[0].astype(f32)
    grid_im = grid[1].astype(f32)
    half_re = jnp.einsum('ky,pyx->pkx', cosf, grid_re) + jnp.einsum('ky,pyx->pkx', sinf, grid_im)
    half_im = jnp.einsum('ky,pyx->pkx', cosf, grid_im) - jnp.einsum('ky,pyx->pkx', sinf, grid_re)
    half_re = half_re.astype(jnp.bfloat16).astype(f32)
    half_im = half_im.astype(jnp.bfloat16).astype(f32)
    out_re = jnp.einsum('pkx,mx->pkm', half_re, cosf) + jnp.einsum('pkx,mx->pkm', half_im, sinf)
    out_im = jnp.einsum('pkx,mx->pkm', half_im, cosf) - jnp.einsum('pkx,mx->pkm', half_re, sinf)
    return jnp.stack([out_re, out_im])

def conj_product(sens, image):
    real_part = sens[0] * image[0] + sens[1] * image[1]
    imag_part = sens[0] * image[1] - sens[1] * image[0]
    return jnp.stack([real_part, imag_part])

def reference(kdata, spoke_angle, spoke_count, block_index, interp, sens_maps):
    cos_t, sin_t = dft_tables(N, jnp.bfloat16)
    weights = spoke_weights(spoke_count, spoke_angle, ANGLES, SPOKES)

    def per_coil(total, coil_id):
        data = lax.dynamic_index_in_dim(kdata, coil_id, 2, keepdims=False)
        image_c = coil_image(data, weights, interp, block_index, cos_t, sin_t)
        sens = lax.dynamic_index_in_dim(sens_maps, coil_id, 1, keepdims=False).astype(jnp.float32)
        return (total + conj_product(sens[:, None], image_c), None)
    start = jnp.zeros((2, KZ, N, N), jnp.float32)
    combined, unused = lax.scan(per_coil, start, jnp.arange(COILS, dtype=jnp.int32))
    cos_z, sin_z = dft_tables(KZ, jnp.float32)
    high = lax.Precision.HIGHEST
    image_re = jnp.einsum('zk,kyx->zyx', cos_z, combined[0], precision=high) + jnp.einsum('zk,kyx->zyx', sin_z, combined[1], precision=high)
    image_im = jnp.einsum('zk,kyx->zyx', cos_z, combined[1], precision=high) - jnp.einsum('zk,kyx->zyx', sin_z, combined[0], precision=high)
    return jnp.stack([image_re, image_im])
```

```python
import functools
import math

import jax
import jax.numpy as jnp
import numpy as np
from jax import lax
from jax.experimental import pallas as pl
from jax.experimental.pallas import tpu as pltpu
from jax.sharding import PartitionSpec as P

F32 = jnp.float32
BF16 = jnp.bfloat16
I32 = jnp.int32
SUB = 2
SUBLANE, LANE = 8, 128
CUTS = 4
LAG = 2


def cos_sin(product, length):
    phase = (product % length).astype(np.float64) * (2.0 * np.pi / length)
    scale = 1.0 / np.sqrt(length)
    return np.cos(phase) * scale, np.sin(phase) * scale


def halving_orders(bits):
    first = list(range(bits))
    return [first, first[:1] + first[:0:-1]]


def plan(steps, batches, per_batch):
    if steps == 4 and batches == 4 and per_batch == 2:
        half = CUTS // 2
        bins = {0: 0, 4: 1, 7: 2, 9: 3}
        cuts = {0: (0, 0, CUTS), 4: (1, 0, CUTS), 7: (2, 0, half), 8: (2, half, CUTS), 10: (3, 0, CUTS)}
        pairs = {1: (0, 1), 2: (1, 2), 5: (2, 3), 6: (3, 4), 8: (4, 5), 9: (5, 6), 11: (6, 8)}
        items = [(0, s) for s in range(4)] + [(1 + k // 2, k % 2) for k in range(6)] + [(1 + k % 3, 2 + k // 3) for k in range(6)]
        return bins, cuts, pairs, items, [k + 3 if k < 4 else k + 4 for k in range(16)]
    items = [(b, s) for b in range(batches) for s in range(steps)]
    bins = {2 * b: b for b in range(batches)}
    cuts = {2 * b: (b, 0, CUTS) for b in range(batches)}
    pairs = {2 * b + 1: (b * per_batch, (b + 1) * per_batch) for b in range(batches)}
    return bins, cuts, pairs, items, [2 * batches + k for k in range(len(items))]


def kernel(dims, *refs):
    bits, groups, parts, rows, side, angles, segs, seg, spokes = dims
    kdata_in, angle_in, count_in, where_in, interp_in, sens_in, dft_in, twiddle_in, out_hbm = refs[:9]
    kdata, angle, count, where, interp, sens, dft, twiddle = refs[9:17]
    ymat, xmat, match, binned, contrib = refs[17:22]
    weighted, raw, part_out, part_in = refs[22:26]
    inbox = refs[26 : 26 + bits]
    out, small_sem, data_sem, interp_sem, out_sem = refs[26 + bits : 31 + bits]
    sent, first_recv, half_recv, line_recv = refs[31 + bits :]
    blocks = 1 << bits
    orders = halving_orders(bits)
    lanes = side // LANE
    steps = rows // SUBLANE
    share = SUBLANE // 2
    batches = parts // share
    per_batch = share // SUB
    hits = angles * segs
    pitch = hits + SUBLANE
    coil = lax.axis_index("coil")
    kz = lax.axis_index("kz")
    my_bit = [(coil // (1 << bit)) % 2 for bit in range(bits)]
    partner = [coil + (1 - 2 * my_bit[bit]) * (1 << bit) for bit in range(bits)]
    last = groups - 1
    inner = (kz > 0) & (kz < last)
    outer = (kz == 0) | (kz == last)
    inward = jnp.where(kz < 2, kz + 1, kz - 1)
    outward = jnp.where(kz < 2, 0, last)

    smalls = [
        pltpu.make_async_copy(src, dst, small_sem.at[i])
        for i, (src, dst) in enumerate(
            ((angle_in, angle), (count_in, count), (where_in, where), (dft_in, dft), (sens_in, sens), (twiddle_in, twiddle))
        )
    ]

    def data_copy(batch):
        span = pl.ds(batch * share, share)
        return pltpu.make_async_copy(kdata_in.at[:, span], kdata.at[:, span], data_sem.at[batch])

    per_cut = angles // CUTS

    def interp_copy(cut):
        span = pl.ds(cut * per_cut, per_cut)
        return pltpu.make_async_copy(interp_in.at[span], interp.at[span], interp_sem.at[cut])

    for copy in smalls[:2]:
        copy.start()
    data_copy(0).start()
    for copy in smalls[2:]:
        copy.start()
    for cut in range(2):
        interp_copy(cut).start()

    barrier = pltpu.get_barrier_semaphore()
    for bit in range(bits):
        pl.semaphore_signal(barrier, 1, device_id={"coil": partner[bit]})
    pl.semaphore_signal(barrier, 1, device_id={"kz": (kz + 1) % groups})
    pl.semaphore_signal(barrier, 1, device_id={"kz": (kz + groups - 1) % groups})

    out[...] = jnp.zeros_like(out)
    part_out[...] = jnp.zeros_like(part_out)

    for copy in smalls[:2]:
        copy.wait()
    match[...] = (angle[...] == lax.broadcasted_iota(I32, (angles, spokes), 0)).astype(F32)
    for copy in smalls[2:]:
        copy.wait()
    for cut in range(2, CUTS):
        interp_copy(cut).start()
    for batch in range(1, batches):
        data_copy(batch).start()
    across = side // seg
    row = lax.broadcasted_iota(I32, (side, hits), 0) * across
    hit_at = jnp.concatenate([where[g : g + 1, :] for g in range(segs)], axis=1)
    for h in range(across):
        here = (hit_at == row + h).astype(F32).astype(BF16)
        for r in range(2):
            part = jnp.dot(dft[r], here, preferred_element_type=F32)
            if r == 0:
                ymat[h, :side, :hits] = part.astype(BF16)
                ymat[h, side:, hits:] = part.astype(BF16)
            else:
                ymat[h, :side, hits:] = part.astype(BF16)
                ymat[h, side:, :hits] = (-part).astype(BF16)
    cos_x, sin_x = dft[0], dft[1]
    xmat[:side, :side] = cos_x
    xmat[:side, side:] = -sin_x
    xmat[side:, :side] = sin_x
    xmat[side:, side:] = cos_x

    def kept_start(order, stage):
        start = 0
        for s in range(stage):
            start = start + my_bit[order[s]] * (blocks >> (s + 1))
        return start

    half = blocks // 2

    def first_copy(step, span, arrived):
        chunk = pl.ds(step * lanes, lanes)
        return pltpu.make_async_remote_copy(
            src_ref=weighted.at[chunk, pl.ds((1 - my_bit[0]) * half, half), span],
            dst_ref=inbox[0].at[chunk, :, span],
            send_sem=sent.at[0],
            recv_sem=first_recv.at[arrived, step],
            device_id={"coil": partner[0]},
        )

    def first_of_pair(pair, step):
        return first_copy(step, pl.ds(pair * SUB, SUB), pair // per_batch)

    def first_of_batch(batch, step):
        return first_copy(step, of(batch), batch)

    def all_first():
        return pltpu.make_async_remote_copy(
            src_ref=weighted.at[:, pl.ds(0, half)],
            dst_ref=inbox[0],
            send_sem=sent.at[0],
            recv_sem=first_recv.at[0, 0],
            device_id={"coil": partner[0]},
        )

    def of(batch):
        return pl.ds(batch * share, share)

    def half_copy(batch, step, lane, stage):
        order = orders[lane % 2]
        bit = order[stage]
        size = blocks >> (stage + 1)
        start = kept_start(order, stage) + (1 - my_bit[bit]) * size
        chunk = step * lanes + lane
        return pltpu.make_async_remote_copy(
            src_ref=weighted.at[chunk, pl.ds(start, size), of(batch)],
            dst_ref=inbox[stage].at[chunk, :, of(batch)],
            send_sem=sent.at[stage],
            recv_sem=half_recv.at[stage - 1, batch, step],
            device_id={"coil": partner[bit]},
        )

    def half_of_step(batch, step, stage):
        size = blocks >> (stage + 1)
        chunk = pl.ds(step * lanes, lanes)
        return pltpu.make_async_remote_copy(
            src_ref=weighted.at[chunk, pl.ds(0, size), of(batch)],
            dst_ref=inbox[stage].at[chunk, :, of(batch)],
            send_sem=sent.at[stage],
            recv_sem=half_recv.at[stage - 1, batch, step],
            device_id={"coil": partner[stage]},
        )

    def all_half(stage):
        return pltpu.make_async_remote_copy(
            src_ref=weighted.at[:, pl.ds(0, blocks >> (stage + 1))],
            dst_ref=inbox[stage],
            send_sem=sent.at[stage],
            recv_sem=half_recv.at[stage - 1, 0, 0],
            device_id={"coil": partner[stage]},
        )

    def add_inbox(batch, step, lane, stage):
        size = blocks >> (stage + 1)
        start = kept_start(orders[lane % 2], stage + 1)
        chunk = step * lanes + lane
        for b in range(size):
            total = weighted[chunk, start + b, of(batch)] + inbox[stage][chunk, b, of(batch)]
            if stage < bits - 1:
                weighted[chunk, start + b, of(batch)] = total
            else:
                raw[step, kz, lane, of(batch)] = total

    def raw_copy(batch, step, source, leaves, lands):
        return pltpu.make_async_remote_copy(
            src_ref=raw.at[step, source, :, of(batch)],
            dst_ref=raw.at[step, source, :, of(batch)],
            send_sem=sent.at[bits + leaves],
            recv_sem=line_recv.at[lands, batch, step],
            device_id={"kz": inward},
        )

    def from_outer(batch, step, source):
        return raw_copy(batch, step, source, 0, 0)

    def from_inner(batch, step, source):
        return raw_copy(batch, step, source, 0, 1)

    def forward(batch, step, source):
        return raw_copy(batch, step, source, 1, 1)

    def far_side(batch, step):
        return raw_copy(batch, step, pl.ds(jnp.where(kz < 2, 2, 0), 2), 0, 1)

    def all_raw(source, leaves):
        return pltpu.make_async_remote_copy(
            src_ref=raw.at[:, source],
            dst_ref=raw.at[:, source],
            send_sem=sent.at[bits + leaves],
            recv_sem=line_recv.at[0, 0, 0],
            device_id={"kz": inward},
        )

    def partial(step, lane):
        return pltpu.make_async_remote_copy(
            src_ref=part_out.at[step, lane],
            dst_ref=part_in.at[step, lane],
            send_sem=sent.at[bits + 2],
            recv_sem=line_recv.at[0, lane, step],
            device_id={"kz": outward},
        )

    def all_partial():
        return pltpu.make_async_remote_copy(
            src_ref=part_out,
            dst_ref=part_in,
            send_sem=sent.at[bits + 2],
            recv_sem=line_recv.at[0, 0, 0],
            device_id={"kz": outward},
        )

    def bin_batch(batch):
        data_copy(batch).wait()
        spot = lax.broadcasted_iota(I32, (angles, spokes), 1)
        for i in range(share):
            p = batch * share + i
            weights = jnp.where(spot < count[p], match[...], 0.0).astype(BF16)
            for r in range(2):
                total = jnp.dot(weights, kdata[r, p], preferred_element_type=F32)
                for g in range(segs):
                    binned[g, pl.ds(i * 2 + r, angles, stride=SUBLANE), :] = total[:, g * seg : (g + 1) * seg]

    def interpolate(batch, cut):
        @pl.when(batch == 0)
        def _():
            interp_copy(cut).wait()

        empty = jnp.zeros((2 * SUBLANE, seg), BF16)
        for pair in range(per_cut // 2):
            a = cut * per_cut + pair * 2
            rows_at = pl.ds(pl.multiple_of(a * SUBLANE, 2 * SUBLANE), 2 * SUBLANE)
            for g in range(0, segs, 2):
                low, high = [binned[g + i, rows_at, :].astype(BF16) for i in range(2)]
                rows_in = jnp.concatenate(
                    [jnp.concatenate([low, empty], axis=1), jnp.concatenate([empty, high], axis=1)], axis=0
                )
                matrix = jnp.concatenate(
                    [jnp.concatenate([interp[a, g + i], interp[a + 1, g + i]], axis=1) for i in range(2)], axis=0
                )
                both = jnp.dot(rows_in, matrix, preferred_element_type=F32)
                for i in range(2):
                    for j in range(2):
                        top = (2 * i + j) * SUBLANE
                        hit = (g + i) * angles + a + j
                        contrib[batch, pl.ds(hit, SUBLANE, stride=pitch), :] = both[top : top + SUBLANE, j * seg : (j + 1) * seg]

    def compute(pair):
        first = pair * SUB
        batch = pair // per_batch
        at = (pair % per_batch) * SUB

        def column(s):
            tops = [pl.multiple_of(((at + s) * 2 + r) * pitch, SUBLANE) for r in range(2)]
            return jnp.concatenate([contrib[batch, pl.ds(top, hits), :] for top in tops], axis=0).astype(BF16)

        data = jnp.concatenate([column(s) for s in range(SUB)], axis=1)
        halves = [jnp.dot(ymat[h], data, preferred_element_type=F32).astype(BF16) for h in range(across)]
        s_re = sens[0].astype(F32)
        s_im = sens[1].astype(F32)
        for s in range(SUB):
            pieces = [h[r * side : (r + 1) * side, s * seg : (s + 1) * seg] for r in range(2) for h in halves]
            image = jnp.dot(jnp.concatenate(pieces, axis=1), xmat[...], preferred_element_type=F32)
            i_re, i_im = image[:, :side], image[:, side:]
            result = [s_re * i_re + s_im * i_im, s_re * i_im - s_im * i_re]
            for block in range(blocks):
                for lane in range(lanes):
                    place = 0
                    for bit in orders[lane % 2]:
                        place = place * 2 + (block >> bit) % 2
                    for step in range(steps):
                        top = block * rows + step * SUBLANE
                        for r in range(2):
                            weighted[step * lanes + lane, place, first + s, r] = result[r][
                                top : top + SUBLANE, lane * LANE : (lane + 1) * LANE
                            ]

    def transform(batch, step, lane, sources, owner, load, store):
        for q in range(groups):
            sums = []
            for i in range(share):
                re = im = None
                for j in sources:
                    turn = 2.0 * math.pi * (q * j % groups) / groups
                    c, d = round(math.cos(turn), 12), round(math.sin(turn), 12)
                    k = batch * share + i
                    x_re, x_im = raw[step, j, lane, k, 0], raw[step, j, lane, k, 1]
                    for coef, a, b in ((c, x_re, x_im), (d, x_im, -x_re)):
                        if coef == 0.0:
                            continue
                        ta = a if coef == 1.0 else a * F32(coef)
                        tb = b if coef == 1.0 else b * F32(coef)
                        re = ta if re is None else re + ta
                        im = tb if im is None else im + tb
                sums.append((re, im))
            for z in range(q, parts, groups):
                a_re, a_im = load(z)
                for i in range(share):
                    spot = (owner * parts + batch * share + i) * 2 * parts + z
                    c, d = twiddle[spot], twiddle[spot + parts]
                    re, im = sums[i]
                    a_re = a_re + (c * re + d * im)
                    a_im = a_im + (c * im - d * re)
                store(z, a_re, a_im)

    def spot(step, lane):
        return pl.ds(pl.multiple_of(step * SUBLANE, SUBLANE), SUBLANE), pl.ds(lane * LANE, LANE)

    def in_out(step, lane):
        y, x = spot(step, lane)

        def load(z):
            return out[0, z, y, x], out[1, z, y, x]

        def store(z, re, im):
            out[0, z, y, x] = re
            out[1, z, y, x] = im

        return load, store

    def in_partial(step, lane):
        def load(z):
            return part_out[step, lane, z, 0], part_out[step, lane, z, 1]

        def store(z, re, im):
            part_out[step, lane, z, 0] = re
            part_out[step, lane, z, 1] = im

        return load, store

    def reduce_stage(stage, batch, step):
        if stage == 0:
            first_of_batch(batch, step).wait_recv()
        else:
            half_of_step(batch, step, stage).wait_recv()

        for lane in range(lanes):
            add_inbox(batch, step, lane, stage)
            if stage < bits - 1:
                half_copy(batch, step, lane, stage + 1).start()
        if stage == bits - 1:

            @pl.when(outer)
            def _():
                from_outer(batch, step, kz).start()

            @pl.when(inner)
            def _():
                from_inner(batch, step, kz).start()

    def relay_stage(batch, step):
        @pl.when(inner)
        def _():
            from_outer(batch, step, outward).wait_recv()
            forward(batch, step, outward).start()

        for end in (0, last):

            @pl.when(kz == end)
            def _(end=end):
                for lane in range(lanes):
                    transform(batch, step, lane, [end], kz, *in_out(step, lane))

    def combine_stage(batch, step):
        @pl.when(inner)
        def _():
            far_side(batch, step).wait_recv()

        for place, end in ((1, 0), (last - 1, last)):

            @pl.when(kz == place)
            def _(end=end):
                for lane in range(lanes):
                    transform(batch, step, lane, [j for j in range(groups) if j != end], outward, *in_partial(step, lane))

                    @pl.when(batch == batches - 1)
                    def _():
                        partial(step, lane).start()

        @pl.when(inner)
        def _():
            for lane in range(lanes):
                transform(batch, step, lane, list(range(groups)), kz, *in_out(step, lane))

            @pl.when(batch == batches - 1)
            def _():
                out_copy(step).start()

    def out_copy(step):
        y = pl.ds(step * SUBLANE, SUBLANE)
        return pltpu.make_async_copy(out.at[:, :, y], out_hbm.at[:, :, y], out_sem.at[0])

    def finish(step):
        @pl.when(outer)
        def _():
            for lane in range(lanes):
                partial(step, lane).wait_recv()
                y, x = spot(step, lane)
                for r in range(2):
                    out[r, :, y, x] = out[r, :, y, x] + part_in[step, lane, :, r]
            out_copy(step).start()

    bins, cuts, pair_at, items, starts = plan(steps, batches, per_batch)

    def pick(t, table):
        value = 0
        for key, entry in table.items():
            value = value + jnp.where(t == key, entry, 0)
        return value

    def tick(t, carry):
        def at(lag, body):
            when = [start + lag for start in starts]
            found = pick(t, {k: 1 for k in when})
            batch = pick(t, {k: item[0] for k, item in zip(when, items)})
            step = pick(t, {k: item[1] for k, item in zip(when, items)})

            @pl.when(found > 0)
            def _():
                body(batch, step)

        at(LAG * bits, relay_stage)
        for stage in range(bits - 1, -1, -1):
            at(LAG * stage, functools.partial(reduce_stage, stage))

        @pl.when(pick(t, {k: 1 for k in bins}) > 0)
        def _():
            bin_batch(pick(t, bins))

        batch, low, high = [pick(t, {k: v[i] for k, v in cuts.items()}) for i in range(3)]

        def one_cut(cut, carry):
            interpolate(batch, cut)
            return carry

        lax.fori_loop(low, high, one_cut, 0)
        first, end = [pick(t, {k: v[i] for k, v in pair_at.items()}) for i in range(2)]

        def one_pair(pair, carry):
            compute(pair)
            for step in range(steps):
                first_of_pair(pair, step).start()
            return carry

        lax.fori_loop(first, end, one_pair, 0)
        at(LAG * bits + LAG, combine_stage)
        return carry

    pl.semaphore_wait(barrier, bits + 2)
    lax.fori_loop(0, starts[-1] + LAG * bits + LAG + 1, tick, 0)

    def finish_early(step, carry):
        finish(step)
        return carry

    lax.fori_loop(0, steps - 1, finish_early, 0)

    all_first().wait_send()
    for stage in range(1, bits):
        all_half(stage).wait_send()
    all_raw(kz, 0).wait_send()
    finish(steps - 1)

    @pl.when(inner)
    def _():
        all_raw(outward, 1).wait_send()
        all_partial().wait_send()

    pltpu.make_async_copy(out, out_hbm, out_sem.at[0]).wait()


def per_device(kdata, spoke_angle, spoke_count, block_index, interp, sens_maps):
    side = sens_maps.shape[2]
    parts = kdata.shape[1]
    spokes, samples = kdata.shape[3:]
    angles, segs, seg = interp.shape[:3]
    coils = lax.axis_size("coil")
    groups = lax.axis_size("kz")
    bits = coils.bit_length() - 1
    rows = side // coils
    hits = angles * segs
    share = SUBLANE // 2
    batches = parts // share
    steps = rows // SUBLANE
    lanes = side // LANE
    across = side // seg

    assert groups == 4 and parts % groups == 0 and parts % share == 0 and angles % (2 * CUTS) == 0 and segs % 2 == 0
    index = np.arange(side)
    dft = jnp.asarray(np.stack(cos_sin(index[:, None] * index[None, :], side)), BF16)
    low = np.arange(parts)
    tables = []
    for owner in range(groups):
        pair = cos_sin(low[:, None] * (owner * parts + low)[None, :], parts * groups)
        tables.append(np.stack(pair, 1))
    twiddle = jnp.asarray(np.stack(tables).reshape(-1), F32)

    chunks = steps * lanes
    block = (parts, 2, SUBLANE, LANE)
    vmem = pltpu.VMEM
    scratch = [
        vmem((2, parts, spokes, samples), BF16),
        vmem((1, spokes), I32),
        pltpu.SMEM((parts,), I32),
        vmem((segs, angles), I32),
        vmem((angles, segs, seg, seg), BF16),
        vmem((2, side, side), BF16),
        vmem((2, side, side), BF16),
        pltpu.SMEM(twiddle.shape, F32),
        vmem((across, 2 * side, 2 * hits), BF16),
        vmem((2 * side, 2 * side), BF16),
        vmem((angles, spokes), F32),
        vmem((segs, angles * SUBLANE, seg), F32),
        vmem((batches, 2 * share * (hits + SUBLANE), seg), F32),
        vmem((chunks, coils) + block, F32),
        vmem((steps, groups, lanes) + block, F32),
        vmem((steps, lanes) + block, F32),
        vmem((steps, lanes) + block, F32),
    ]
    scratch += [vmem((chunks, coils >> (s + 1)) + block, F32) for s in range(bits)]
    dma = pltpu.SemaphoreType.DMA
    scratch += [vmem((2, parts, rows, side), F32)]
    scratch += [dma((6,)), dma((batches,)), dma((CUTS,)), dma((1,))]
    scratch += [dma((bits + 3,)), dma((batches, steps)), dma((bits - 1, batches, steps)), dma((2, batches, steps))]
    anywhere = pl.BlockSpec(memory_space=pltpu.HBM)
    dims = (bits, groups, parts, rows, side, angles, segs, seg, spokes)
    return pl.pallas_call(
        functools.partial(kernel, dims),
        out_shape=jax.ShapeDtypeStruct((2, parts, rows, side), F32),
        in_specs=[anywhere] * 8,
        out_specs=anywhere,
        scratch_shapes=scratch,
        compiler_params=pltpu.CompilerParams(
            collective_id=0, has_side_effects=True, vmem_limit_bytes=60 * 1024 * 1024
        ),
        name="reconstruct",
    )(
        kdata[:, :, 0],
        spoke_angle.reshape(1, -1),
        spoke_count,
        block_index.T,
        interp,
        sens_maps[:, 0],
        dft,
        twiddle,
    )


def solution(mesh):
    placed = (
        P(None, "kz", "coil", None, None),
        P(),
        P("kz"),
        P(),
        P(),
        P(None, "coil", None, None),
    )
    return jax.shard_map(
        per_device,
        mesh=mesh,
        in_specs=placed,
        out_specs=P(None, "kz", "coil", None),
        check_vma=False,
    )
```

```python
import functools
import math

import jax
import jax.numpy as jnp
import numpy as np
from jax import lax
from jax.experimental import pallas as pl
from jax.experimental.pallas import tpu as pltpu
from jax.sharding import PartitionSpec as P

F32 = jnp.float32
BF16 = jnp.bfloat16
I32 = jnp.int32
SUB = 2
SUBLANE, LANE = 8, 128
CUTS = 4
LAG = 3


def cos_sin(product, length):
    phase = (product % length).astype(np.float64) * (2.0 * np.pi / length)
    scale = 1.0 / np.sqrt(length)
    return np.cos(phase) * scale, np.sin(phase) * scale


def halving_orders(bits):
    first = list(range(bits))
    return [first, first[:1] + first[:0:-1]]


def plan(chunks, batches, per_batch):
    if chunks == 8 and batches == 4 and per_batch == 2 and CUTS == 4:
        bins = {0: 0, 4: 1, 9: 2, 14: 3}
        cuts = {0: (0, 0, 4)}
        for b, t in ((1, 4), (2, 9), (3, 14)):
            cuts |= {t: (b, 0, 1), t + 1: (b, 1, 3), t + 2: (b, 3, 4)}
        pairs = {1: (0, 1), 2: (1, 2), 7: (2, 3), 8: (3, 4), 11: (4, 5), 12: (5, 6), 16: (6, 7), 17: (7, 8)}
        return bins, cuts, pairs, 3, True
    bins = {2 * b: b for b in range(batches)}
    cuts = {2 * b: (b, 0, CUTS) for b in range(batches)}
    pairs = {2 * b + 1: (b * per_batch, (b + 1) * per_batch) for b in range(batches)}
    return bins, cuts, pairs, 2 * batches, False


def nth_item(k, chunks, mixed):
    if not mixed:
        return lax.div(k, chunks), lax.rem(k, chunks)
    a, b, c = [jnp.maximum(k, first) - first for first in (8, 20, 26)]
    late_batch = jnp.where(k < 26, 1 + lax.div(b, 2), 1 + lax.rem(c, 3))
    late_chunk = jnp.where(k < 26, 4 + lax.rem(b, 2), 6 + lax.div(c, 3))
    batch = jnp.where(k < 8, 0, jnp.where(k < 20, 1 + lax.div(a, 4), late_batch))
    chunk = jnp.where(k < 8, k, jnp.where(k < 20, lax.rem(a, 4), late_chunk))
    return batch, chunk


def kernel(dims, *refs):
    bits, groups, parts, rows, side, angles, segs, seg, spokes = dims
    kdata_in, angle_in, count_in, where_in, interp_in, sens_in, dft_in, twiddle_in, out = refs[:9]
    kdata, angle, count, where, interp, sens, dft, twiddle = refs[9:17]
    ymat, xmat, match, binned, contrib = refs[17:22]
    weighted, raw, part_out, part_in = refs[22:26]
    inbox = refs[26 : 26 + bits]
    small_sem, data_sem, interp_sem = refs[26 + bits : 29 + bits]
    sent, first_recv, half_recv, line_recv = refs[29 + bits :]
    blocks = 1 << bits
    orders = halving_orders(bits)
    lanes = side // LANE
    steps = rows // SUBLANE
    chunks = steps * lanes
    share = SUBLANE // 2
    batches = parts // share
    per_batch = share // SUB
    hits = angles * segs
    pitch = hits + SUBLANE
    coil = lax.axis_index("coil")
    kz = lax.axis_index("kz")
    my_bit = [(coil // (1 << bit)) % 2 for bit in range(bits)]
    partner = [coil + (1 - 2 * my_bit[bit]) * (1 << bit) for bit in range(bits)]
    last = groups - 1
    inner = (kz > 0) & (kz < last)
    outer = (kz == 0) | (kz == last)
    inward = jnp.where(kz < 2, kz + 1, kz - 1)
    outward = jnp.where(kz < 2, 0, last)

    smalls = [
        pltpu.make_async_copy(src, dst, small_sem.at[i])
        for i, (src, dst) in enumerate(
            ((angle_in, angle), (count_in, count), (where_in, where), (dft_in, dft), (sens_in, sens), (twiddle_in, twiddle))
        )
    ]

    def data_copy(batch):
        span = pl.ds(batch * share, share)
        return pltpu.make_async_copy(kdata_in.at[:, span], kdata.at[:, span], data_sem.at[batch])

    per_cut = angles // CUTS

    def interp_copy(cut):
        span = pl.ds(cut * per_cut, per_cut)
        return pltpu.make_async_copy(interp_in.at[span], interp.at[span], interp_sem.at[cut])

    for copy in smalls[:2]:
        copy.start()
    data_copy(0).start()
    for copy in smalls[2:]:
        copy.start()
    for cut in range(2):
        interp_copy(cut).start()

    barrier = pltpu.get_barrier_semaphore()
    for bit in range(bits):
        pl.semaphore_signal(barrier, 1, device_id={"coil": partner[bit]})
    pl.semaphore_signal(barrier, 1, device_id={"kz": (kz + 1) % groups})
    pl.semaphore_signal(barrier, 1, device_id={"kz": (kz + groups - 1) % groups})

    out[...] = jnp.zeros_like(out)
    part_out[...] = jnp.zeros_like(part_out)

    for copy in smalls[:2]:
        copy.wait()
    match[...] = (angle[...] == lax.broadcasted_iota(I32, (angles, spokes), 0)).astype(F32)
    for copy in smalls[2:]:
        copy.wait()
    for cut in range(2, CUTS):
        interp_copy(cut).start()
    for batch in range(1, batches):
        data_copy(batch).start()
    across = side // seg
    row = lax.broadcasted_iota(I32, (side, hits), 0) * across
    hit_at = jnp.concatenate([where[g : g + 1, :] for g in range(segs)], axis=1)
    for h in range(across):
        here = (hit_at == row + h).astype(F32).astype(BF16)
        for r in range(2):
            part = jnp.dot(dft[r], here, preferred_element_type=F32)
            if r == 0:
                ymat[h, :side, :hits] = part.astype(BF16)
                ymat[h, side:, hits:] = part.astype(BF16)
            else:
                ymat[h, :side, hits:] = part.astype(BF16)
                ymat[h, side:, :hits] = (-part).astype(BF16)
    cos_x, sin_x = dft[0], dft[1]
    xmat[:side, :side] = cos_x
    xmat[:side, side:] = -sin_x
    xmat[side:, :side] = sin_x
    xmat[side:, side:] = cos_x

    def kept_start(order, stage):
        start = 0
        for s in range(stage):
            start = start + my_bit[order[s]] * (blocks >> (s + 1))
        return start

    half = blocks // 2

    def of(batch):
        return pl.ds(batch * per_batch, per_batch)

    def first_copy(step, span, arrived):
        chunk = pl.ds(step * lanes, lanes)
        return pltpu.make_async_remote_copy(
            src_ref=weighted.at[chunk, pl.ds((1 - my_bit[0]) * half, half), :, span],
            dst_ref=inbox[0].at[chunk, :, :, span],
            send_sem=sent.at[0],
            recv_sem=first_recv.at[arrived, step],
            device_id={"coil": partner[0]},
        )

    def first_of_pair(pair, step):
        return first_copy(step, pl.ds(pair, 1), pair // per_batch)

    def first_of_batch(batch, step):
        return first_copy(step, of(batch), batch)

    def all_first():
        return pltpu.make_async_remote_copy(
            src_ref=weighted.at[:, pl.ds(0, half)],
            dst_ref=inbox[0],
            send_sem=sent.at[0],
            recv_sem=first_recv.at[0, 0],
            device_id={"coil": partner[0]},
        )

    def half_copy(batch, chunk, way, stage):
        order = orders[way]
        bit = order[stage]
        size = blocks >> (stage + 1)
        start = kept_start(order, stage) + (1 - my_bit[bit]) * size
        return pltpu.make_async_remote_copy(
            src_ref=weighted.at[chunk, pl.ds(start, size), way, of(batch)],
            dst_ref=inbox[stage].at[chunk, :, way, of(batch)],
            send_sem=sent.at[stage],
            recv_sem=half_recv.at[stage - 1, batch, chunk],
            device_id={"coil": partner[bit]},
        )

    def both_halves(batch, chunk, stage):
        return pltpu.make_async_remote_copy(
            src_ref=weighted.at[chunk, pl.ds(0, blocks >> (stage + 1)), :, of(batch)],
            dst_ref=inbox[stage].at[chunk, :, :, of(batch)],
            send_sem=sent.at[stage],
            recv_sem=half_recv.at[stage - 1, batch, chunk],
            device_id={"coil": partner[stage]},
        )

    def all_half(stage):
        return pltpu.make_async_remote_copy(
            src_ref=weighted.at[:, pl.ds(0, blocks >> (stage + 1))],
            dst_ref=inbox[stage],
            send_sem=sent.at[stage],
            recv_sem=half_recv.at[stage - 1, 0, 0],
            device_id={"coil": partner[stage]},
        )

    def add_inbox(batch, chunk, way, stage):
        size = blocks >> (stage + 1)
        start = kept_start(orders[way], stage + 1)
        for b in range(size):
            total = weighted[chunk, start + b, way, of(batch)] + inbox[stage][chunk, b, way, of(batch)]
            if stage < bits - 1:
                weighted[chunk, start + b, way, of(batch)] = total
            else:
                raw[chunk, kz, way, of(batch)] = total

    def raw_copy(batch, chunk, source, leaves, lands):
        return pltpu.make_async_remote_copy(
            src_ref=raw.at[chunk, source, :, of(batch)],
            dst_ref=raw.at[chunk, source, :, of(batch)],
            send_sem=sent.at[bits + leaves],
            recv_sem=line_recv.at[lands, batch, chunk],
            device_id={"kz": inward},
        )

    def from_outer(batch, chunk, source):
        return raw_copy(batch, chunk, source, 0, 0)

    def from_inner(batch, chunk, source):
        return raw_copy(batch, chunk, source, 0, 1)

    def forward(batch, chunk, source):
        return raw_copy(batch, chunk, source, 1, 1)

    def far_side(batch, chunk):
        far = pl.ds(jnp.where(kz < 2, 2, 0), 2)
        return pltpu.make_async_remote_copy(
            src_ref=raw.at[chunk, far, :, of(batch)],
            dst_ref=raw.at[chunk, far, :, of(batch)],
            send_sem=sent.at[bits],
            recv_sem=line_recv.at[1, batch, chunk],
            device_id={"kz": inward},
        )

    def all_raw(source, leaves):
        return pltpu.make_async_remote_copy(
            src_ref=raw.at[:, source],
            dst_ref=raw.at[:, source],
            send_sem=sent.at[bits + leaves],
            recv_sem=line_recv.at[0, 0, 0],
            device_id={"kz": inward},
        )

    def partial(chunk):
        return pltpu.make_async_remote_copy(
            src_ref=part_out.at[chunk],
            dst_ref=part_in.at[chunk],
            send_sem=sent.at[bits + 2],
            recv_sem=line_recv.at[0, 0, chunk],
            device_id={"kz": outward},
        )

    def all_partial():
        return pltpu.make_async_remote_copy(
            src_ref=part_out,
            dst_ref=part_in,
            send_sem=sent.at[bits + 2],
            recv_sem=line_recv.at[0, 0, 0],
            device_id={"kz": outward},
        )

    def bin_batch(batch):
        data_copy(batch).wait()
        spot = lax.broadcasted_iota(I32, (angles, spokes), 1)
        for i in range(share):
            p = batch * share + i
            weights = jnp.where(spot < count[p], match[...], 0.0).astype(BF16)
            for r in range(2):
                total = jnp.dot(weights, kdata[r, p], preferred_element_type=F32)
                for g in range(segs):
                    binned[g, pl.ds(i * 2 + r, angles, stride=SUBLANE), :] = total[:, g * seg : (g + 1) * seg]

    def interpolate(batch, cut):
        @pl.when(batch == 0)
        def _():
            interp_copy(cut).wait()

        empty = jnp.zeros((2 * SUBLANE, seg), BF16)
        for pair in range(per_cut // 2):
            a = cut * per_cut + pair * 2
            rows_at = pl.ds(pl.multiple_of(a * SUBLANE, 2 * SUBLANE), 2 * SUBLANE)
            for g in range(0, segs, 2):
                low, high = [binned[g + i, rows_at, :].astype(BF16) for i in range(2)]
                rows_in = jnp.concatenate(
                    [jnp.concatenate([low, empty], axis=1), jnp.concatenate([empty, high], axis=1)], axis=0
                )
                matrix = jnp.concatenate(
                    [jnp.concatenate([interp[a, g + i], interp[a + 1, g + i]], axis=1) for i in range(2)], axis=0
                )
                both = jnp.dot(rows_in, matrix, preferred_element_type=F32)
                for i in range(2):
                    for j in range(2):
                        top = (2 * i + j) * SUBLANE
                        hit = (g + i) * angles + a + j
                        contrib[batch, pl.ds(hit, SUBLANE, stride=pitch), :] = both[top : top + SUBLANE, j * seg : (j + 1) * seg]

    def compute(pair):
        batch = pair // per_batch
        at = (pair % per_batch) * SUB

        def column(s):
            tops = [pl.multiple_of(((at + s) * 2 + r) * pitch, SUBLANE) for r in range(2)]
            return jnp.concatenate([contrib[batch, pl.ds(top, hits), :] for top in tops], axis=0).astype(BF16)

        data = jnp.concatenate([column(s) for s in range(SUB)], axis=1)
        halves = [jnp.dot(ymat[h], data, preferred_element_type=F32).astype(BF16) for h in range(across)]
        s_re = sens[0].astype(F32)
        s_im = sens[1].astype(F32)
        for s in range(SUB):
            pieces = [h[r * side : (r + 1) * side, s * seg : (s + 1) * seg] for r in range(2) for h in halves]
            image = jnp.dot(jnp.concatenate(pieces, axis=1), xmat[...], preferred_element_type=F32)
            i_re, i_im = image[:, :side], image[:, side:]
            result = [s_re * i_re + s_im * i_im, s_re * i_im - s_im * i_re]
            for block in range(blocks):
                place = 0
                for bit in orders[s % 2]:
                    place = place * 2 + (block >> bit) % 2
                for lane in range(lanes):
                    for step in range(steps):
                        top = block * rows + step * SUBLANE
                        for r in range(2):
                            weighted[step * lanes + lane, place, s, pair, r] = result[r][
                                top : top + SUBLANE, lane * LANE : (lane + 1) * LANE
                            ]

    def transform(batch, chunk, sources, owner, load, store):
        for q in range(groups):
            sums = []
            for i in range(share):
                re = im = None
                for j in sources:
                    turn = 2.0 * math.pi * (q * j % groups) / groups
                    c, d = round(math.cos(turn), 12), round(math.sin(turn), 12)
                    x_re, x_im = [raw[chunk, j, i % SUB, batch * per_batch + i // SUB, r] for r in range(2)]
                    for coef, a, b in ((c, x_re, x_im), (d, x_im, -x_re)):
                        if coef == 0.0:
                            continue
                        ta = a if coef == 1.0 else a * F32(coef)
                        tb = b if coef == 1.0 else b * F32(coef)
                        re = ta if re is None else re + ta
                        im = tb if im is None else im + tb
                sums.append((re, im))
            for z in range(q, parts, groups):
                a_re, a_im = load(z)
                for i in range(share):
                    spot = (owner * parts + batch * share + i) * 2 * parts + z
                    c, d = twiddle[spot], twiddle[spot + parts]
                    re, im = sums[i]
                    a_re = a_re + (c * re + d * im)
                    a_im = a_im + (c * im - d * re)
                store(z, a_re, a_im)

    def spot(chunk):
        y = pl.multiple_of(lax.div(chunk, lanes) * SUBLANE, SUBLANE)
        x = pl.multiple_of(lax.rem(chunk, lanes) * LANE, LANE)
        return pl.ds(y, SUBLANE), pl.ds(x, LANE)

    def in_out(chunk):
        y, x = spot(chunk)

        def load(z):
            return out[0, z, y, x], out[1, z, y, x]

        def store(z, re, im):
            out[0, z, y, x] = re
            out[1, z, y, x] = im

        return load, store

    def in_partial(chunk):
        def load(z):
            return part_out[chunk, z, 0], part_out[chunk, z, 1]

        def store(z, re, im):
            part_out[chunk, z, 0] = re
            part_out[chunk, z, 1] = im

        return load, store

    def reduce_stage(stage, batch, chunk):
        if stage == 0:

            @pl.when(lax.rem(chunk, lanes) == 0)
            def _():
                first_of_batch(batch, lax.div(chunk, lanes)).wait_recv()
        else:
            both_halves(batch, chunk, stage).wait_recv()
        for way in range(2):
            add_inbox(batch, chunk, way, stage)
            if stage < bits - 1:
                half_copy(batch, chunk, way, stage + 1).start()
        if stage == bits - 1:

            @pl.when(outer)
            def _():
                from_outer(batch, chunk, kz).start()

            @pl.when(inner)
            def _():
                from_inner(batch, chunk, kz).start()

    def relay_stage(batch, chunk):
        @pl.when(inner)
        def _():
            from_outer(batch, chunk, outward).wait_recv()
            forward(batch, chunk, outward).start()

        for end in (0, last):

            @pl.when(kz == end)
            def _(end=end):
                transform(batch, chunk, [end], kz, *in_out(chunk))

    def combine_stage(batch, chunk):
        @pl.when(inner)
        def _():
            far_side(batch, chunk).wait_recv()

        for place, end in ((1, 0), (last - 1, last)):

            @pl.when(kz == place)
            def _(end=end):
                transform(batch, chunk, [j for j in range(groups) if j != end], outward, *in_partial(chunk))

                @pl.when(batch == batches - 1)
                def _():
                    partial(chunk).start()

        @pl.when(inner)
        def _():
            transform(batch, chunk, list(range(groups)), kz, *in_out(chunk))

    def finish(chunk):
        @pl.when(outer)
        def _():
            partial(chunk).wait_recv()
            y, x = spot(chunk)
            for r in range(2):
                out[r, :, y, x] = out[r, :, y, x] + part_in[chunk, :, r]

    bins, cuts, pair_at, begin, mixed = plan(chunks, batches, per_batch)
    count_items = batches * chunks

    def pick(t, table):
        value = 0
        for key, entry in table.items():
            value = value + jnp.where(t == key, entry, 0)
        return value

    def tick(t, carry):
        def at(lag, body):
            start = begin + lag
            k = jnp.minimum(jnp.maximum(t, start) - start, count_items - 1)
            batch, chunk = nth_item(k, chunks, mixed)

            @pl.when((t >= start) & (t < start + count_items))
            def _():
                body(batch, chunk)

        at(LAG * bits, relay_stage)
        for stage in range(bits - 1, -1, -1):
            at(LAG * stage, functools.partial(reduce_stage, stage))

        @pl.when(pick(t, {k: 1 for k in bins}) > 0)
        def _():
            bin_batch(pick(t, bins))

        batch, low, high = [pick(t, {k: v[i] for k, v in cuts.items()}) for i in range(3)]

        def one_cut(cut, carry):
            interpolate(batch, cut)
            return carry

        lax.fori_loop(low, high, one_cut, 0)
        first, end = [pick(t, {k: v[i] for k, v in pair_at.items()}) for i in range(2)]

        def one_pair(pair, carry):
            compute(pair)
            for step in range(steps):
                first_of_pair(pair, step).start()
            return carry

        lax.fori_loop(first, end, one_pair, 0)
        at(LAG * bits + LAG, combine_stage)
        return carry

    pl.semaphore_wait(barrier, bits + 2)
    lax.fori_loop(0, begin + count_items + LAG * bits + LAG, tick, 0)

    def finish_early(chunk, carry):
        finish(chunk)
        return carry

    lax.fori_loop(0, chunks - 1, finish_early, 0)

    all_first().wait_send()
    for stage in range(1, bits):
        all_half(stage).wait_send()
    all_raw(kz, 0).wait_send()
    finish(chunks - 1)

    @pl.when(inner)
    def _():
        all_raw(outward, 1).wait_send()
        all_partial().wait_send()


def per_device(kdata, spoke_angle, spoke_count, block_index, interp, sens_maps):
    side = sens_maps.shape[2]
    parts = kdata.shape[1]
    spokes, samples = kdata.shape[3:]
    angles, segs, seg = interp.shape[:3]
    coils = lax.axis_size("coil")
    groups = lax.axis_size("kz")
    bits = coils.bit_length() - 1
    rows = side // coils
    hits = angles * segs
    share = SUBLANE // 2
    batches = parts // share
    steps = rows // SUBLANE
    lanes = side // LANE
    across = side // seg

    assert groups == 4 and parts % groups == 0 and parts % share == 0 and angles % (2 * CUTS) == 0 and segs % 2 == 0
    index = np.arange(side)
    dft = jnp.asarray(np.stack(cos_sin(index[:, None] * index[None, :], side)), BF16)
    low = np.arange(parts)
    tables = []
    for owner in range(groups):
        pair = cos_sin(low[:, None] * (owner * parts + low)[None, :], parts * groups)
        tables.append(np.stack(pair, 1))
    twiddle = jnp.asarray(np.stack(tables).reshape(-1), F32)

    chunks = steps * lanes
    block = (parts, 2, SUBLANE, LANE)
    by_way = (2, parts // SUB, 2, SUBLANE, LANE)
    vmem = pltpu.VMEM
    scratch = [
        vmem((2, parts, spokes, samples), BF16),
        vmem((1, spokes), I32),
        pltpu.SMEM((parts,), I32),
        vmem((segs, angles), I32),
        vmem((angles, segs, seg, seg), BF16),
        vmem((2, side, side), BF16),
        vmem((2, side, side), BF16),
        pltpu.SMEM(twiddle.shape, F32),
        vmem((across, 2 * side, 2 * hits), BF16),
        vmem((2 * side, 2 * side), BF16),
        vmem((angles, spokes), F32),
        vmem((segs, angles * SUBLANE, seg), F32),
        vmem((batches, 2 * share * (hits + SUBLANE), seg), F32),
        vmem((chunks, coils) + by_way, F32),
        vmem((chunks, groups) + by_way, F32),
        vmem((chunks,) + block, F32),
        vmem((chunks,) + block, F32),
    ]
    scratch += [vmem((chunks, coils >> (s + 1)) + by_way, F32) for s in range(bits)]
    dma = pltpu.SemaphoreType.DMA
    scratch += [dma((6,)), dma((batches,)), dma((CUTS,))]
    scratch += [dma((bits + 3,)), dma((batches, steps)), dma((bits - 1, batches, chunks)), dma((2, batches, chunks))]
    anywhere = pl.BlockSpec(memory_space=pltpu.HBM)
    dims = (bits, groups, parts, rows, side, angles, segs, seg, spokes)
    return pl.pallas_call(
        functools.partial(kernel, dims),
        out_shape=pltpu.VMEM((2, parts, rows, side), F32),
        in_specs=[anywhere] * 8,
        out_specs=pl.BlockSpec(memory_space=pltpu.VMEM),
        scratch_shapes=scratch,
        compiler_params=pltpu.CompilerParams(
            collective_id=0, has_side_effects=True, vmem_limit_bytes=60 * 1024 * 1024
        ),
        name="reconstruct",
    )(
        kdata[:, :, 0],
        spoke_angle.reshape(1, -1),
        spoke_count,
        block_index.T,
        interp,
        sens_maps[:, 0],
        dft,
        twiddle,
    )


def solution(mesh):
    placed = (
        P(None, "kz", "coil", None, None),
        P(),
        P("kz"),
        P(),
        P(),
        P(None, "coil", None, None),
    )
    return jax.shard_map(
        per_device,
        mesh=mesh,
        in_specs=placed,
        out_specs=P(None, "kz", "coil", None),
        check_vma=False,
    )
```

```python
import functools
import math

import jax
import jax.numpy as jnp
import numpy as np
from jax import lax
from jax.experimental import pallas as pl
from jax.experimental.pallas import tpu as pltpu
from jax.sharding import PartitionSpec as P

F32 = jnp.float32
BF16 = jnp.bfloat16
I32 = jnp.int32
SUB = 2
SUBLANE, LANE = 8, 128
CUTS = 4
LAG = 3
HALF_SLOTS, INNER_SLOTS = 8, 16


def cos_sin(product, length):
    phase = (product % length).astype(np.float64) * (2.0 * np.pi / length)
    scale = 1.0 / np.sqrt(length)
    return np.cos(phase) * scale, np.sin(phase) * scale


def halving_orders(bits):
    first = list(range(bits))
    return [first, first[:1] + first[:0:-1]]


def plan(chunks, batches, per_batch):
    if chunks == 8 and batches == 4 and per_batch == 2 and CUTS == 4:
        bins = {0: 0, 4: 1, 9: 2, 14: 3}
        cuts = {0: (0, 0, 4)}
        for b, t in ((1, 4), (2, 9), (3, 14)):
            cuts |= {t: (b, 0, 1), t + 1: (b, 1, 3), t + 2: (b, 3, 4)}
        pairs = {1: (0, 1), 2: (1, 2), 7: (2, 3), 8: (3, 4), 11: (4, 5), 12: (5, 6), 16: (6, 7), 17: (7, 8)}
        return bins, cuts, pairs, 3, True
    bins = {2 * b: b for b in range(batches)}
    cuts = {2 * b: (b, 0, CUTS) for b in range(batches)}
    pairs = {2 * b + 1: (b * per_batch, (b + 1) * per_batch) for b in range(batches)}
    return bins, cuts, pairs, 2 * batches, False


def nth_item(k, chunks, mixed):
    if not mixed:
        return lax.div(k, chunks), lax.rem(k, chunks)
    a, b, c = [jnp.maximum(k, first) - first for first in (8, 20, 26)]
    late_batch = jnp.where(k < 26, 1 + lax.div(b, 2), 1 + lax.rem(c, 3))
    late_chunk = jnp.where(k < 26, 4 + lax.rem(b, 2), 6 + lax.div(c, 3))
    batch = jnp.where(k < 8, 0, jnp.where(k < 20, 1 + lax.div(a, 4), late_batch))
    chunk = jnp.where(k < 8, k, jnp.where(k < 20, lax.rem(a, 4), late_chunk))
    return batch, chunk


def kernel(dims, *refs):
    bits, groups, parts, rows, side, angles, segs, seg, spokes = dims
    kdata_in, angle_in, count_in, where_in, interp_in, sens_in, dft_in, twiddle_in, out = refs[:9]
    kdata, angle, count, where, interp, sens, dft, twiddle = refs[9:17]
    ymat, xmat, match, binned, contrib = refs[17:22]
    weighted, raw, part_out, part_in = refs[22:26]
    inbox = refs[26 : 26 + bits]
    small_sem, data_sem, interp_sem = refs[26 + bits : 29 + bits]
    sent, first_recv, half_recv, outer_recv, inner_recv = refs[29 + bits :]
    blocks = 1 << bits
    orders = halving_orders(bits)
    lanes = side // LANE
    steps = rows // SUBLANE
    chunks = steps * lanes
    share = SUBLANE // 2
    batches = parts // share
    per_batch = share // SUB
    hits = angles * segs
    pitch = hits + SUBLANE
    coil = lax.axis_index("coil")
    kz = lax.axis_index("kz")
    my_bit = [(coil // (1 << bit)) % 2 for bit in range(bits)]
    partner = [coil + (1 - 2 * my_bit[bit]) * (1 << bit) for bit in range(bits)]
    last = groups - 1
    inner = (kz > 0) & (kz < last)
    outer = (kz == 0) | (kz == last)
    inward = jnp.where(kz < 2, kz + 1, kz - 1)
    outward = jnp.where(kz < 2, 0, last)

    smalls = [
        pltpu.make_async_copy(src, dst, small_sem.at[i])
        for i, (src, dst) in enumerate(
            ((angle_in, angle), (count_in, count), (where_in, where), (dft_in, dft), (sens_in, sens), (twiddle_in, twiddle))
        )
    ]

    def data_copy(batch):
        span = pl.ds(batch * share, share)
        return pltpu.make_async_copy(kdata_in.at[:, span], kdata.at[:, span], data_sem.at[batch])

    per_cut = angles // CUTS

    def interp_copy(cut):
        span = pl.ds(cut * per_cut, per_cut)
        return pltpu.make_async_copy(interp_in.at[span], interp.at[span], interp_sem.at[cut])

    for copy in smalls[:2]:
        copy.start()
    data_copy(0).start()
    for copy in smalls[2:]:
        copy.start()

    barrier = pltpu.get_barrier_semaphore()
    for bit in range(bits):
        pl.semaphore_signal(barrier, 1, device_id={"coil": partner[bit]})
    pl.semaphore_signal(barrier, 1, device_id={"kz": (kz + 1) % groups})
    pl.semaphore_signal(barrier, 1, device_id={"kz": (kz + groups - 1) % groups})

    out[...] = jnp.zeros_like(out)
    part_out[...] = jnp.zeros_like(part_out)

    for copy in smalls[:2]:
        copy.wait()
    interp_copy(0).start()
    match[...] = (angle[...] == lax.broadcasted_iota(I32, (angles, spokes), 0)).astype(F32)
    for copy in smalls[2:]:
        copy.wait()
    for cut in range(1, CUTS):
        interp_copy(cut).start()
    across = side // seg
    row = lax.broadcasted_iota(I32, (side, hits), 0) * across
    hit_at = jnp.concatenate([where[g : g + 1, :] for g in range(segs)], axis=1)
    for h in range(across):
        here = (hit_at == row + h).astype(F32).astype(BF16)
        for r in range(2):
            part = jnp.dot(dft[r], here, preferred_element_type=F32)
            if r == 0:
                ymat[h, :side, :hits] = part.astype(BF16)
                ymat[h, side:, hits:] = part.astype(BF16)
            else:
                ymat[h, :side, hits:] = part.astype(BF16)
                ymat[h, side:, :hits] = (-part).astype(BF16)
    cos_x, sin_x = dft[0], dft[1]
    xmat[:side, :side] = cos_x
    xmat[:side, side:] = -sin_x
    xmat[side:, :side] = sin_x
    xmat[side:, side:] = cos_x

    def kept_start(order, stage):
        start = 0
        for s in range(stage):
            start = start + my_bit[order[s]] * (blocks >> (s + 1))
        return start

    half = blocks // 2

    def of(batch):
        return pl.ds(batch * per_batch, per_batch)

    def first_of_step(step, span):
        chunk = pl.ds(step * lanes, lanes)
        return pltpu.make_async_remote_copy(
            src_ref=weighted.at[chunk, pl.ds((1 - my_bit[0]) * half, half), :, span],
            dst_ref=inbox[0].at[chunk, :, :, span],
            send_sem=sent.at[0],
            recv_sem=first_recv.at[step],
            device_id={"coil": partner[0]},
        )

    def first_whole(batch, span):
        return pltpu.make_async_remote_copy(
            src_ref=weighted.at[:, pl.ds((1 - my_bit[0]) * half, half), :, span],
            dst_ref=inbox[0].at[:, :, :, span],
            send_sem=sent.at[0],
            recv_sem=first_recv.at[steps + batch],
            device_id={"coil": partner[0]},
        )

    def all_first():
        return pltpu.make_async_remote_copy(
            src_ref=weighted.at[:, pl.ds(0, half)],
            dst_ref=inbox[0],
            send_sem=sent.at[0],
            recv_sem=first_recv.at[0],
            device_id={"coil": partner[0]},
        )

    def half_copy(batch, chunk, k, way, stage):
        order = orders[way]
        bit = order[stage]
        size = blocks >> (stage + 1)
        start = kept_start(order, stage) + (1 - my_bit[bit]) * size
        return pltpu.make_async_remote_copy(
            src_ref=weighted.at[chunk, pl.ds(start, size), way, of(batch)],
            dst_ref=inbox[stage].at[chunk, :, way, of(batch)],
            send_sem=sent.at[stage],
            recv_sem=half_recv.at[stage - 1, lax.rem(k, HALF_SLOTS)],
            device_id={"coil": partner[bit]},
        )

    def both_halves(batch, chunk, k, stage):
        return pltpu.make_async_remote_copy(
            src_ref=weighted.at[chunk, pl.ds(0, blocks >> (stage + 1)), :, of(batch)],
            dst_ref=inbox[stage].at[chunk, :, :, of(batch)],
            send_sem=sent.at[stage],
            recv_sem=half_recv.at[stage - 1, lax.rem(k, HALF_SLOTS)],
            device_id={"coil": partner[stage]},
        )

    def all_half(stage):
        return pltpu.make_async_remote_copy(
            src_ref=weighted.at[:, pl.ds(0, blocks >> (stage + 1))],
            dst_ref=inbox[stage],
            send_sem=sent.at[stage],
            recv_sem=half_recv.at[stage - 1, 0],
            device_id={"coil": partner[stage]},
        )

    def add_inbox(batch, chunk, way, stage):
        size = blocks >> (stage + 1)
        start = kept_start(orders[way], stage + 1)
        for b in range(size):
            total = weighted[chunk, start + b, way, of(batch)] + inbox[stage][chunk, b, way, of(batch)]
            if stage < bits - 1:
                weighted[chunk, start + b, way, of(batch)] = total
            else:
                raw[chunk, kz, way, of(batch)] = total

    def raw_copy(batch, chunk, source, leaves, landed):
        return pltpu.make_async_remote_copy(
            src_ref=raw.at[chunk, source, :, of(batch)],
            dst_ref=raw.at[chunk, source, :, of(batch)],
            send_sem=sent.at[bits + leaves],
            recv_sem=landed,
            device_id={"kz": inward},
        )

    def from_outer(batch, chunk, k, source):
        return raw_copy(batch, chunk, source, 0, outer_recv.at[k])

    def from_inner(batch, chunk, k, source):
        return raw_copy(batch, chunk, source, 0, inner_recv.at[lax.rem(k, INNER_SLOTS)])

    def forward(batch, chunk, k, source):
        return raw_copy(batch, chunk, source, 1, inner_recv.at[lax.rem(k, INNER_SLOTS)])

    def far_side(batch, chunk, k):
        far = pl.ds(jnp.where(kz < 2, 2, 0), 2)
        return pltpu.make_async_remote_copy(
            src_ref=raw.at[chunk, far, :, of(batch)],
            dst_ref=raw.at[chunk, far, :, of(batch)],
            send_sem=sent.at[bits],
            recv_sem=inner_recv.at[lax.rem(k, INNER_SLOTS)],
            device_id={"kz": inward},
        )

    def all_raw(source, leaves):
        return pltpu.make_async_remote_copy(
            src_ref=raw.at[:, source],
            dst_ref=raw.at[:, source],
            send_sem=sent.at[bits + leaves],
            recv_sem=outer_recv.at[0],
            device_id={"kz": inward},
        )

    def partial(chunk):
        return pltpu.make_async_remote_copy(
            src_ref=part_out.at[chunk],
            dst_ref=part_in.at[chunk],
            send_sem=sent.at[bits + 2],
            recv_sem=outer_recv.at[chunk],
            device_id={"kz": outward},
        )

    def all_partial():
        return pltpu.make_async_remote_copy(
            src_ref=part_out,
            dst_ref=part_in,
            send_sem=sent.at[bits + 2],
            recv_sem=outer_recv.at[0],
            device_id={"kz": outward},
        )

    def bin_batch(batch):
        data_copy(batch).wait()
        spot = lax.broadcasted_iota(I32, (angles, spokes), 1)
        for i in range(share):
            p = batch * share + i
            weights = jnp.where(spot < count[p], match[...], 0.0).astype(BF16)
            for r in range(2):
                total = jnp.dot(weights, kdata[r, p], preferred_element_type=F32)
                for g in range(segs):
                    binned[g, pl.ds(i * 2 + r, angles, stride=SUBLANE), :] = total[:, g * seg : (g + 1) * seg]

    def interpolate(batch, cut):
        @pl.when(batch == 0)
        def _():
            interp_copy(cut).wait()

        empty = jnp.zeros((2 * SUBLANE, seg), BF16)
        for pair in range(per_cut // 2):
            a = cut * per_cut + pair * 2
            rows_at = pl.ds(pl.multiple_of(a * SUBLANE, 2 * SUBLANE), 2 * SUBLANE)
            for g in range(0, segs, 2):
                low, high = [binned[g + i, rows_at, :].astype(BF16) for i in range(2)]
                rows_in = jnp.concatenate(
                    [jnp.concatenate([low, empty], axis=1), jnp.concatenate([empty, high], axis=1)], axis=0
                )
                matrix = jnp.concatenate(
                    [jnp.concatenate([interp[a, g + i], interp[a + 1, g + i]], axis=1) for i in range(2)], axis=0
                )
                both = jnp.dot(rows_in, matrix, preferred_element_type=F32)
                for i in range(2):
                    for j in range(2):
                        top = (2 * i + j) * SUBLANE
                        hit = (g + i) * angles + a + j
                        contrib[batch, pl.ds(hit, SUBLANE, stride=pitch), :] = both[top : top + SUBLANE, j * seg : (j + 1) * seg]

    def compute(pair):
        batch = pair // per_batch
        at = (pair % per_batch) * SUB

        def column(s):
            tops = [pl.multiple_of(((at + s) * 2 + r) * pitch, SUBLANE) for r in range(2)]
            return jnp.concatenate([contrib[batch, pl.ds(top, hits), :] for top in tops], axis=0).astype(BF16)

        data = jnp.concatenate([column(s) for s in range(SUB)], axis=1)
        halves = [jnp.dot(ymat[h], data, preferred_element_type=F32).astype(BF16) for h in range(across)]
        s_re = sens[0].astype(F32)
        s_im = sens[1].astype(F32)
        for s in range(SUB):
            pieces = [h[r * side : (r + 1) * side, s * seg : (s + 1) * seg] for r in range(2) for h in halves]
            image = jnp.dot(jnp.concatenate(pieces, axis=1), xmat[...], preferred_element_type=F32)
            i_re, i_im = image[:, :side], image[:, side:]
            result = [s_re * i_re + s_im * i_im, s_re * i_im - s_im * i_re]
            for block in range(blocks):
                place = 0
                for bit in orders[s % 2]:
                    place = place * 2 + (block >> bit) % 2
                for lane in range(lanes):
                    for step in range(steps):
                        top = block * rows + step * SUBLANE
                        for r in range(2):
                            weighted[step * lanes + lane, place, s, pair, r] = result[r][
                                top : top + SUBLANE, lane * LANE : (lane + 1) * LANE
                            ]

    def transform(batch, chunk, sources, owner, load, store):
        for q in range(groups):
            sums = []
            for i in range(share):
                re = im = None
                for j in sources:
                    turn = 2.0 * math.pi * (q * j % groups) / groups
                    c, d = round(math.cos(turn), 12), round(math.sin(turn), 12)
                    x_re, x_im = [raw[chunk, j, i % SUB, batch * per_batch + i // SUB, r] for r in range(2)]
                    for coef, a, b in ((c, x_re, x_im), (d, x_im, -x_re)):
                        if coef == 0.0:
                            continue
                        ta = a if coef == 1.0 else a * F32(coef)
                        tb = b if coef == 1.0 else b * F32(coef)
                        re = ta if re is None else re + ta
                        im = tb if im is None else im + tb
                sums.append((re, im))
            for z in range(q, parts, groups):
                a_re, a_im = load(z)
                for i in range(share):
                    spot = (owner * parts + batch * share + i) * 2 * parts + z
                    c, d = twiddle[spot], twiddle[spot + parts]
                    re, im = sums[i]
                    a_re = a_re + (c * re + d * im)
                    a_im = a_im + (c * im - d * re)
                store(z, a_re, a_im)

    def spot(chunk):
        y = pl.multiple_of(lax.div(chunk, lanes) * SUBLANE, SUBLANE)
        x = pl.multiple_of(lax.rem(chunk, lanes) * LANE, LANE)
        return pl.ds(y, SUBLANE), pl.ds(x, LANE)

    def in_out(chunk):
        y, x = spot(chunk)

        def load(z):
            return out[0, z, y, x], out[1, z, y, x]

        def store(z, re, im):
            out[0, z, y, x] = re
            out[1, z, y, x] = im

        return load, store

    def in_partial(chunk):
        def load(z):
            return part_out[chunk, z, 0], part_out[chunk, z, 1]

        def store(z, re, im):
            part_out[chunk, z, 0] = re
            part_out[chunk, z, 1] = im

        return load, store

    def reduce_stage(stage, batch, chunk, k):
        if stage == 0:

            @pl.when((batch == 0) & (lax.rem(chunk, lanes) == 0))
            def _():
                first_of_step(lax.div(chunk, lanes), of(0)).wait_recv()

            @pl.when((batch > 0) & (chunk == 0))
            def _():
                first_whole(batch, of(batch)).wait_recv()

        else:
            both_halves(batch, chunk, k, stage).wait_recv()
        for way in range(2):
            add_inbox(batch, chunk, way, stage)
            if stage < bits - 1:
                half_copy(batch, chunk, k, way, stage + 1).start()
        if stage == bits - 1:

            @pl.when(outer)
            def _():
                from_outer(batch, chunk, k, kz).start()

            @pl.when(inner)
            def _():
                from_inner(batch, chunk, k, kz).start()

    def relay_stage(batch, chunk, k):
        @pl.when(inner)
        def _():
            from_outer(batch, chunk, k, outward).wait_recv()
            forward(batch, chunk, k, outward).start()

        for end in (0, last):

            @pl.when(kz == end)
            def _(end=end):
                transform(batch, chunk, [end], kz, *in_out(chunk))

    def combine_stage(batch, chunk, k):
        @pl.when(inner)
        def _():
            far_side(batch, chunk, k).wait_recv()

        for place, end in ((1, 0), (last - 1, last)):

            @pl.when(kz == place)
            def _(end=end):
                transform(batch, chunk, [j for j in range(groups) if j != end], outward, *in_partial(chunk))

                @pl.when(batch == batches - 1)
                def _():
                    partial(chunk).start()

        @pl.when(inner)
        def _():
            transform(batch, chunk, list(range(groups)), kz, *in_out(chunk))

    def finish(chunk):
        @pl.when(outer)
        def _():
            partial(chunk).wait_recv()
            y, x = spot(chunk)
            for r in range(2):
                out[r, :, y, x] = out[r, :, y, x] + part_in[chunk, :, r]

    bins, cuts, pair_at, begin, mixed = plan(chunks, batches, per_batch)
    count_items = batches * chunks

    def pick(t, table):
        value = 0
        for key, entry in table.items():
            value = value + jnp.where(t == key, entry, 0)
        return value

    def tick(t, carry):
        def at(lag, body):
            start = begin + lag
            k = jnp.minimum(jnp.maximum(t, start) - start, count_items - 1)
            batch, chunk = nth_item(k, chunks, mixed)

            @pl.when((t >= start) & (t < start + count_items))
            def _():
                body(batch, chunk, k)

        at(LAG * bits, relay_stage)
        for stage in range(bits - 1, -1, -1):
            at(LAG * stage, functools.partial(reduce_stage, stage))

        @pl.when(pick(t, {k: 1 for k in bins}) > 0)
        def _():
            bin_batch(pick(t, bins))

        batch, low, high = [pick(t, {k: v[i] for k, v in cuts.items()}) for i in range(3)]

        def one_cut(cut, carry):
            interpolate(batch, cut)
            return carry

        lax.fori_loop(low, high, one_cut, 0)

        @pl.when(t == 0)
        def _():
            for later in range(1, batches):
                data_copy(later).start()

        first, end = [pick(t, {k: v[i] for k, v in pair_at.items()}) for i in range(2)]

        def one_pair(pair, carry):
            compute(pair)
            batch = pair // per_batch

            @pl.when(batch == 0)
            def _():
                for step in range(steps):
                    first_of_step(step, pl.ds(pair, 1)).start()

            @pl.when(batch > 0)
            def _():
                first_whole(batch, pl.ds(pair, 1)).start()

            return carry

        lax.fori_loop(first, end, one_pair, 0)
        at(LAG * bits + LAG, combine_stage)
        return carry

    pl.semaphore_wait(barrier, bits + 2)
    lax.fori_loop(0, begin + count_items + LAG * bits + LAG, tick, 0)

    def finish_early(chunk, carry):
        finish(chunk)
        return carry

    lax.fori_loop(0, chunks - 1, finish_early, 0)

    all_first().wait_send()
    for stage in range(1, bits):
        all_half(stage).wait_send()
    all_raw(kz, 0).wait_send()
    finish(chunks - 1)

    @pl.when(inner)
    def _():
        all_raw(outward, 1).wait_send()
        all_partial().wait_send()


def per_device(kdata, spoke_angle, spoke_count, block_index, interp, sens_maps):
    side = sens_maps.shape[2]
    parts = kdata.shape[1]
    spokes, samples = kdata.shape[3:]
    angles, segs, seg = interp.shape[:3]
    coils = lax.axis_size("coil")
    groups = lax.axis_size("kz")
    bits = coils.bit_length() - 1
    rows = side // coils
    hits = angles * segs
    share = SUBLANE // 2
    batches = parts // share
    steps = rows // SUBLANE
    lanes = side // LANE
    across = side // seg

    assert groups == 4 and parts % groups == 0 and parts % share == 0 and angles % (2 * CUTS) == 0 and segs % 2 == 0
    index = np.arange(side)
    dft = jnp.asarray(np.stack(cos_sin(index[:, None] * index[None, :], side)), BF16)
    low = np.arange(parts)
    tables = []
    for owner in range(groups):
        pair = cos_sin(low[:, None] * (owner * parts + low)[None, :], parts * groups)
        tables.append(np.stack(pair, 1))
    twiddle = jnp.asarray(np.stack(tables).reshape(-1), F32)

    chunks = steps * lanes
    block = (parts, 2, SUBLANE, LANE)
    by_way = (2, parts // SUB, 2, SUBLANE, LANE)
    vmem = pltpu.VMEM
    scratch = [
        vmem((2, parts, spokes, samples), BF16),
        vmem((1, spokes), I32),
        pltpu.SMEM((parts,), I32),
        vmem((segs, angles), I32),
        vmem((angles, segs, seg, seg), BF16),
        vmem((2, side, side), BF16),
        vmem((2, side, side), BF16),
        pltpu.SMEM(twiddle.shape, F32),
        vmem((across, 2 * side, 2 * hits), BF16),
        vmem((2 * side, 2 * side), BF16),
        vmem((angles, spokes), F32),
        vmem((segs, angles * SUBLANE, seg), F32),
        vmem((batches, 2 * share * (hits + SUBLANE), seg), F32),
        vmem((chunks, coils) + by_way, F32),
        vmem((chunks, groups) + by_way, F32),
        vmem((chunks,) + block, F32),
        vmem((chunks,) + block, F32),
    ]
    scratch += [vmem((chunks, coils >> (s + 1)) + by_way, F32) for s in range(bits)]
    dma = pltpu.SemaphoreType.DMA
    scratch += [dma((6,)), dma((batches,)), dma((CUTS,))]
    scratch += [dma((bits + 3,)), dma((steps + batches,)), dma((bits - 1, HALF_SLOTS))]
    scratch += [dma((batches * chunks,)), dma((INNER_SLOTS,))]
    anywhere = pl.BlockSpec(memory_space=pltpu.HBM)
    dims = (bits, groups, parts, rows, side, angles, segs, seg, spokes)
    return pl.pallas_call(
        functools.partial(kernel, dims),
        out_shape=pltpu.VMEM((2, parts, rows, side), F32),
        in_specs=[anywhere] * 8,
        out_specs=pl.BlockSpec(memory_space=pltpu.VMEM),
        scratch_shapes=scratch,
        compiler_params=pltpu.CompilerParams(
            collective_id=0, has_side_effects=True, vmem_limit_bytes=60 * 1024 * 1024
        ),
        name="reconstruct",
    )(
        kdata[:, :, 0],
        spoke_angle.reshape(1, -1),
        spoke_count,
        block_index.T,
        interp,
        sens_maps[:, 0],
        dft,
        twiddle,
    )


def solution(mesh):
    placed = (
        P(None, "kz", "coil", None, None),
        P(),
        P("kz"),
        P(),
        P(),
        P(None, "coil", None, None),
    )
    return jax.shard_map(
        per_device,
        mesh=mesh,
        in_specs=placed,
        out_specs=P(None, "kz", "coil", None),
        check_vma=False,
    )
```

```python
import functools
import math

import jax
import jax.numpy as jnp
import numpy as np
from jax import lax
from jax.experimental import pallas as pl
from jax.experimental.pallas import tpu as pltpu
from jax.sharding import PartitionSpec as P

F32 = jnp.float32
BF16 = jnp.bfloat16
I32 = jnp.int32
SUB = 2
SUBLANE, LANE = 8, 128
CUTS = 4
LAG = 3
HALF_SLOTS, INNER_SLOTS = 6, 10


def cos_sin(product, length):
    phase = (product % length).astype(np.float64) * (2.0 * np.pi / length)
    scale = 1.0 / np.sqrt(length)
    return np.cos(phase) * scale, np.sin(phase) * scale


def halving_orders(bits):
    first = list(range(bits))
    return [first, first[:1] + first[:0:-1]]


def plan(chunks, batches, per_batch):
    if chunks == 8 and batches == 4 and per_batch == 2 and CUTS == 4:
        bins = {0: 0, 4: 1, 9: 2, 14: 3}
        cuts = {0: (0, 0, 4)}
        for b, t in ((1, 4), (2, 9), (3, 14)):
            cuts |= {t: (b, 0, 1), t + 1: (b, 1, 3), t + 2: (b, 3, 4)}
        pairs = {1: (0, 1), 2: (1, 2), 7: (2, 3), 8: (3, 4), 11: (4, 5), 12: (5, 6), 16: (6, 7), 17: (7, 8)}
        return bins, cuts, pairs, 3, True
    bins = {2 * b: b for b in range(batches)}
    cuts = {2 * b: (b, 0, CUTS) for b in range(batches)}
    pairs = {2 * b + 1: (b * per_batch, (b + 1) * per_batch) for b in range(batches)}
    return bins, cuts, pairs, 2 * batches, False


def nth_item(k, chunks, mixed):
    if not mixed:
        return lax.div(k, chunks), lax.rem(k, chunks)
    a, b = [jnp.maximum(k, first) - first for first in (8, 20)]
    late_batch, late_chunk = 1 + lax.rem(b, 3), 4 + lax.div(b, 3)
    batch = jnp.where(k < 8, 0, jnp.where(k < 20, 1 + lax.div(a, 4), late_batch))
    chunk = jnp.where(k < 8, k, jnp.where(k < 20, lax.rem(a, 4), late_chunk))
    return batch, chunk


def kernel(dims, *refs):
    bits, groups, parts, rows, side, angles, segs, seg, spokes = dims
    kdata_in, angle_in, count_in, where_in, interp_in, sens_in, dft_in, twiddle_in, out = refs[:9]
    kdata, angle, count, where, interp, sens, dft, twiddle = refs[9:17]
    ymat, xmat, match, binned, contrib = refs[17:22]
    weighted, raw, part_out, part_in = refs[22:26]
    inbox = refs[26 : 26 + bits]
    small_sem, data_sem, interp_sem = refs[26 + bits : 29 + bits]
    sent, first_recv, half_recv, outer_recv, inner_recv = refs[29 + bits :]
    blocks = 1 << bits
    orders = halving_orders(bits)
    lanes = side // LANE
    steps = rows // SUBLANE
    chunks = steps * lanes
    share = SUBLANE // 2
    batches = parts // share
    per_batch = share // SUB
    hits = angles * segs
    pitch = hits + SUBLANE
    coil = lax.axis_index("coil")
    kz = lax.axis_index("kz")
    my_bit = [(coil // (1 << bit)) % 2 for bit in range(bits)]
    partner = [coil + (1 - 2 * my_bit[bit]) * (1 << bit) for bit in range(bits)]
    last = groups - 1
    inner = (kz > 0) & (kz < last)
    outer = (kz == 0) | (kz == last)
    inward = jnp.where(kz < 2, kz + 1, kz - 1)
    outward = jnp.where(kz < 2, 0, last)

    smalls = [
        pltpu.make_async_copy(src, dst, small_sem.at[i])
        for i, (src, dst) in enumerate(
            ((angle_in, angle), (count_in, count), (where_in, where), (dft_in, dft), (sens_in, sens), (twiddle_in, twiddle))
        )
    ]

    def data_copy(batch):
        span = pl.ds(batch * share, share)
        return pltpu.make_async_copy(kdata_in.at[:, span], kdata.at[:, span], data_sem.at[batch])

    per_cut = angles // CUTS

    def interp_copy(cut):
        span = pl.ds(cut * per_cut, per_cut)
        return pltpu.make_async_copy(interp_in.at[span], interp.at[span], interp_sem.at[cut])

    for copy in smalls[:2]:
        copy.start()
    data_copy(0).start()
    interp_copy(0).start()
    for copy in smalls[2:]:
        copy.start()

    barrier = pltpu.get_barrier_semaphore()
    for bit in range(bits):
        pl.semaphore_signal(barrier, 1, device_id={"coil": partner[bit]})
    pl.semaphore_signal(barrier, 1, device_id={"kz": (kz + 1) % groups})
    pl.semaphore_signal(barrier, 1, device_id={"kz": (kz + groups - 1) % groups})

    out[...] = jnp.zeros_like(out)
    part_out[...] = jnp.zeros_like(part_out)

    for copy in smalls[:2]:
        copy.wait()
    for cut in range(1, CUTS):
        interp_copy(cut).start()
    match[...] = (angle[...] == lax.broadcasted_iota(I32, (angles, spokes), 0)).astype(F32)
    for copy in smalls[2:]:
        copy.wait()
    across = side // seg
    row = lax.broadcasted_iota(I32, (side, hits), 0) * across
    hit_at = jnp.concatenate([where[g : g + 1, :] for g in range(segs)], axis=1)
    for h in range(across):
        here = (hit_at == row + h).astype(F32).astype(BF16)
        for r in range(2):
            part = jnp.dot(dft[r], here, preferred_element_type=F32)
            if r == 0:
                ymat[h, :side, :hits] = part.astype(BF16)
                ymat[h, side:, hits:] = part.astype(BF16)
            else:
                ymat[h, :side, hits:] = part.astype(BF16)
                ymat[h, side:, :hits] = (-part).astype(BF16)
    cos_x, sin_x = dft[0], dft[1]
    xmat[:side, :side] = cos_x
    xmat[:side, side:] = -sin_x
    xmat[side:, :side] = sin_x
    xmat[side:, side:] = cos_x

    def kept_start(order, stage):
        start = 0
        for s in range(stage):
            start = start + my_bit[order[s]] * (blocks >> (s + 1))
        return start

    half = blocks // 2

    def of(batch):
        return pl.ds(batch * per_batch, per_batch)

    def first_of_step(step, span):
        chunk = pl.ds(step * lanes, lanes)
        return pltpu.make_async_remote_copy(
            src_ref=weighted.at[chunk, pl.ds((1 - my_bit[0]) * half, half), :, span],
            dst_ref=inbox[0].at[chunk, :, :, span],
            send_sem=sent.at[0],
            recv_sem=first_recv.at[step],
            device_id={"coil": partner[0]},
        )

    def first_whole(batch, span):
        return pltpu.make_async_remote_copy(
            src_ref=weighted.at[:, pl.ds((1 - my_bit[0]) * half, half), :, span],
            dst_ref=inbox[0].at[:, :, :, span],
            send_sem=sent.at[0],
            recv_sem=first_recv.at[steps + batch],
            device_id={"coil": partner[0]},
        )

    def all_first():
        return pltpu.make_async_remote_copy(
            src_ref=weighted.at[:, pl.ds(0, half)],
            dst_ref=inbox[0],
            send_sem=sent.at[0],
            recv_sem=first_recv.at[0],
            device_id={"coil": partner[0]},
        )

    def half_copy(batch, chunk, k, way, stage):
        order = orders[way]
        bit = order[stage]
        size = blocks >> (stage + 1)
        start = kept_start(order, stage) + (1 - my_bit[bit]) * size
        return pltpu.make_async_remote_copy(
            src_ref=weighted.at[chunk, pl.ds(start, size), way, of(batch)],
            dst_ref=inbox[stage].at[chunk, :, way, of(batch)],
            send_sem=sent.at[stage],
            recv_sem=half_recv.at[stage - 1, lax.rem(k, HALF_SLOTS)],
            device_id={"coil": partner[bit]},
        )

    def both_halves(batch, chunk, k, stage):
        return pltpu.make_async_remote_copy(
            src_ref=weighted.at[chunk, pl.ds(0, blocks >> (stage + 1)), :, of(batch)],
            dst_ref=inbox[stage].at[chunk, :, :, of(batch)],
            send_sem=sent.at[stage],
            recv_sem=half_recv.at[stage - 1, lax.rem(k, HALF_SLOTS)],
            device_id={"coil": partner[stage]},
        )

    def all_half(stage):
        return pltpu.make_async_remote_copy(
            src_ref=weighted.at[:, pl.ds(0, blocks >> (stage + 1))],
            dst_ref=inbox[stage],
            send_sem=sent.at[stage],
            recv_sem=half_recv.at[stage - 1, 0],
            device_id={"coil": partner[stage]},
        )

    def add_inbox(batch, chunk, way, stage):
        size = blocks >> (stage + 1)
        start = kept_start(orders[way], stage + 1)
        for b in range(size):
            total = weighted[chunk, start + b, way, of(batch)] + inbox[stage][chunk, b, way, of(batch)]
            if stage < bits - 1:
                weighted[chunk, start + b, way, of(batch)] = total
            else:
                raw[chunk, kz, way, of(batch)] = total

    def raw_copy(batch, chunk, source, leaves, landed):
        return pltpu.make_async_remote_copy(
            src_ref=raw.at[chunk, source, :, of(batch)],
            dst_ref=raw.at[chunk, source, :, of(batch)],
            send_sem=sent.at[bits + leaves],
            recv_sem=landed,
            device_id={"kz": inward},
        )

    def from_outer(batch, chunk, k, source):
        return raw_copy(batch, chunk, source, 0, outer_recv.at[k])

    def from_inner(batch, chunk, k, source):
        return raw_copy(batch, chunk, source, 0, inner_recv.at[lax.rem(k, INNER_SLOTS)])

    def forward(batch, chunk, k, source):
        return raw_copy(batch, chunk, source, 1, inner_recv.at[lax.rem(k, INNER_SLOTS)])

    def far_side(batch, chunk, k):
        far = pl.ds(jnp.where(kz < 2, 2, 0), 2)
        return pltpu.make_async_remote_copy(
            src_ref=raw.at[chunk, far, :, of(batch)],
            dst_ref=raw.at[chunk, far, :, of(batch)],
            send_sem=sent.at[bits],
            recv_sem=inner_recv.at[lax.rem(k, INNER_SLOTS)],
            device_id={"kz": inward},
        )

    def all_raw(source, leaves):
        return pltpu.make_async_remote_copy(
            src_ref=raw.at[:, source],
            dst_ref=raw.at[:, source],
            send_sem=sent.at[bits + leaves],
            recv_sem=outer_recv.at[0],
            device_id={"kz": inward},
        )

    def partial(chunk):
        return pltpu.make_async_remote_copy(
            src_ref=part_out.at[chunk],
            dst_ref=part_in.at[chunk],
            send_sem=sent.at[bits + 2],
            recv_sem=outer_recv.at[chunk],
            device_id={"kz": outward},
        )

    def all_partial():
        return pltpu.make_async_remote_copy(
            src_ref=part_out,
            dst_ref=part_in,
            send_sem=sent.at[bits + 2],
            recv_sem=outer_recv.at[0],
            device_id={"kz": outward},
        )

    def bin_batch(batch):
        data_copy(batch).wait()
        spot = lax.broadcasted_iota(I32, (angles, spokes), 1)
        for i in range(share):
            p = batch * share + i
            weights = jnp.where(spot < count[p], match[...], 0.0).astype(BF16)
            for r in range(2):
                total = jnp.dot(weights, kdata[r, p], preferred_element_type=F32)
                for g in range(segs):
                    binned[g, pl.ds(i * 2 + r, angles, stride=SUBLANE), :] = total[:, g * seg : (g + 1) * seg]

    def interpolate(batch, cut):
        @pl.when(batch == 0)
        def _():
            interp_copy(cut).wait()

        empty = jnp.zeros((2 * SUBLANE, seg), BF16)
        for pair in range(per_cut // 2):
            a = cut * per_cut + pair * 2
            rows_at = pl.ds(pl.multiple_of(a * SUBLANE, 2 * SUBLANE), 2 * SUBLANE)
            for g in range(0, segs, 2):
                low, high = [binned[g + i, rows_at, :].astype(BF16) for i in range(2)]
                rows_in = jnp.concatenate(
                    [jnp.concatenate([low, empty], axis=1), jnp.concatenate([empty, high], axis=1)], axis=0
                )
                matrix = jnp.concatenate(
                    [jnp.concatenate([interp[a, g + i], interp[a + 1, g + i]], axis=1) for i in range(2)], axis=0
                )
                both = jnp.dot(rows_in, matrix, preferred_element_type=F32)
                for i in range(2):
                    for j in range(2):
                        top = (2 * i + j) * SUBLANE
                        hit = (g + i) * angles + a + j
                        contrib[batch, pl.ds(hit, SUBLANE, stride=pitch), :] = both[top : top + SUBLANE, j * seg : (j + 1) * seg]

    def compute(pair):
        batch = pair // per_batch
        at = (pair % per_batch) * SUB

        def column(s):
            tops = [pl.multiple_of(((at + s) * 2 + r) * pitch, SUBLANE) for r in range(2)]
            return jnp.concatenate([contrib[batch, pl.ds(top, hits), :] for top in tops], axis=0).astype(BF16)

        data = jnp.concatenate([column(s) for s in range(SUB)], axis=1)
        halves = [jnp.dot(ymat[h], data, preferred_element_type=F32).astype(BF16) for h in range(across)]
        s_re = sens[0].astype(F32)
        s_im = sens[1].astype(F32)
        for s in range(SUB):
            pieces = [h[r * side : (r + 1) * side, s * seg : (s + 1) * seg] for r in range(2) for h in halves]
            image = jnp.dot(jnp.concatenate(pieces, axis=1), xmat[...], preferred_element_type=F32)
            i_re, i_im = image[:, :side], image[:, side:]
            result = [s_re * i_re + s_im * i_im, s_re * i_im - s_im * i_re]
            for block in range(blocks):
                place = 0
                for bit in orders[s % 2]:
                    place = place * 2 + (block >> bit) % 2
                for lane in range(lanes):
                    for step in range(steps):
                        top = block * rows + step * SUBLANE
                        for r in range(2):
                            weighted[step * lanes + lane, place, s, pair, r] = result[r][
                                top : top + SUBLANE, lane * LANE : (lane + 1) * LANE
                            ]

    def transform(batch, chunk, sources, owner, load, store):
        for q in range(groups):
            sums = []
            for i in range(share):
                re = im = None
                for j in sources:
                    turn = 2.0 * math.pi * (q * j % groups) / groups
                    c, d = round(math.cos(turn), 12), round(math.sin(turn), 12)
                    x_re, x_im = [raw[chunk, j, i % SUB, batch * per_batch + i // SUB, r] for r in range(2)]
                    for coef, a, b in ((c, x_re, x_im), (d, x_im, -x_re)):
                        if coef == 0.0:
                            continue
                        ta = a if coef == 1.0 else a * F32(coef)
                        tb = b if coef == 1.0 else b * F32(coef)
                        re = ta if re is None else re + ta
                        im = tb if im is None else im + tb
                sums.append((re, im))
            for z in range(q, parts, groups):
                a_re, a_im = load(z)
                for i in range(share):
                    spot = (owner * parts + batch * share + i) * 2 * parts + z
                    c, d = twiddle[spot], twiddle[spot + parts]
                    re, im = sums[i]
                    a_re = a_re + (c * re + d * im)
                    a_im = a_im + (c * im - d * re)
                store(z, a_re, a_im)

    def spot(chunk):
        y = pl.multiple_of(lax.div(chunk, lanes) * SUBLANE, SUBLANE)
        x = pl.multiple_of(lax.rem(chunk, lanes) * LANE, LANE)
        return pl.ds(y, SUBLANE), pl.ds(x, LANE)

    def in_out(chunk):
        y, x = spot(chunk)

        def load(z):
            return out[0, z, y, x], out[1, z, y, x]

        def store(z, re, im):
            out[0, z, y, x] = re
            out[1, z, y, x] = im

        return load, store

    def in_partial(chunk):
        def load(z):
            return part_out[chunk, z, 0], part_out[chunk, z, 1]

        def store(z, re, im):
            part_out[chunk, z, 0] = re
            part_out[chunk, z, 1] = im

        return load, store

    def reduce_stage(stage, batch, chunk, k):
        if stage == 0:

            @pl.when((batch == 0) & (lax.rem(chunk, lanes) == 0))
            def _():
                first_of_step(lax.div(chunk, lanes), of(0)).wait_recv()

            @pl.when((batch > 0) & (chunk == 0))
            def _():
                first_whole(batch, of(batch)).wait_recv()

        else:
            both_halves(batch, chunk, k, stage).wait_recv()
        for way in range(2):
            add_inbox(batch, chunk, way, stage)
            if stage < bits - 1:
                half_copy(batch, chunk, k, way, stage + 1).start()
        if stage == bits - 1:

            @pl.when(outer)
            def _():
                from_outer(batch, chunk, k, kz).start()

            @pl.when(inner)
            def _():
                from_inner(batch, chunk, k, kz).start()

    def relay_stage(batch, chunk, k):
        @pl.when(inner)
        def _():
            from_outer(batch, chunk, k, outward).wait_recv()
            forward(batch, chunk, k, outward).start()

        for end in (0, last):

            @pl.when(kz == end)
            def _(end=end):
                transform(batch, chunk, [end], kz, *in_out(chunk))

    def combine_stage(batch, chunk, k):
        @pl.when(inner)
        def _():
            far_side(batch, chunk, k).wait_recv()

        for place, end in ((1, 0), (last - 1, last)):

            @pl.when(kz == place)
            def _(end=end):
                transform(batch, chunk, [j for j in range(groups) if j != end], outward, *in_partial(chunk))

                @pl.when(batch == batches - 1)
                def _():
                    partial(chunk).start()

        @pl.when(inner)
        def _():
            transform(batch, chunk, list(range(groups)), kz, *in_out(chunk))

    def finish(chunk):
        @pl.when(outer)
        def _():
            partial(chunk).wait_recv()
            y, x = spot(chunk)
            for r in range(2):
                out[r, :, y, x] = out[r, :, y, x] + part_in[chunk, :, r]

    bins, cuts, pair_at, begin, mixed = plan(chunks, batches, per_batch)
    count_items = batches * chunks

    def pick(t, table):
        value = 0
        for key, entry in table.items():
            value = value + jnp.where(t == key, entry, 0)
        return value

    def tick(t, carry):
        def at(lag, body):
            start = begin + lag
            k = jnp.minimum(jnp.maximum(t, start) - start, count_items - 1)
            batch, chunk = nth_item(k, chunks, mixed)

            @pl.when((t >= start) & (t < start + count_items))
            def _():
                body(batch, chunk, k)

        at(LAG * bits, relay_stage)
        for stage in range(bits - 1, -1, -1):
            at(LAG * stage, functools.partial(reduce_stage, stage))

        @pl.when(pick(t, {k: 1 for k in bins}) > 0)
        def _():
            bin_batch(pick(t, bins))

        batch, low, high = [pick(t, {k: v[i] for k, v in cuts.items()}) for i in range(3)]

        def one_cut(cut, carry):
            interpolate(batch, cut)
            return carry

        lax.fori_loop(low, high, one_cut, 0)

        @pl.when(t == 0)
        def _():
            for later in range(1, batches):
                data_copy(later).start()

        first, end = [pick(t, {k: v[i] for k, v in pair_at.items()}) for i in range(2)]

        def one_pair(pair, carry):
            compute(pair)
            batch = pair // per_batch

            @pl.when(batch == 0)
            def _():
                for step in range(steps):
                    first_of_step(step, pl.ds(pair, 1)).start()

            @pl.when(batch > 0)
            def _():
                first_whole(batch, pl.ds(pair, 1)).start()

            return carry

        lax.fori_loop(first, end, one_pair, 0)
        at(LAG * bits + 2, combine_stage)
        return carry

    pl.semaphore_wait(barrier, bits + 2)
    lax.fori_loop(0, begin + count_items + LAG * bits + LAG, tick, 0)

    def finish_early(chunk, carry):
        finish(chunk)
        return carry

    lax.fori_loop(0, chunks - 1, finish_early, 0)

    all_first().wait_send()
    for stage in range(1, bits):
        all_half(stage).wait_send()
    all_raw(kz, 0).wait_send()
    finish(chunks - 1)

    @pl.when(inner)
    def _():
        all_raw(outward, 1).wait_send()
        all_partial().wait_send()


def per_device(kdata, spoke_angle, spoke_count, block_index, interp, sens_maps):
    side = sens_maps.shape[2]
    parts = kdata.shape[1]
    spokes, samples = kdata.shape[3:]
    angles, segs, seg = interp.shape[:3]
    coils = lax.axis_size("coil")
    groups = lax.axis_size("kz")
    bits = coils.bit_length() - 1
    rows = side // coils
    hits = angles * segs
    share = SUBLANE // 2
    batches = parts // share
    steps = rows // SUBLANE
    lanes = side // LANE
    across = side // seg

    assert groups == 4 and parts % groups == 0 and parts % share == 0 and angles % (2 * CUTS) == 0 and segs % 2 == 0
    index = np.arange(side)
    dft = jnp.asarray(np.stack(cos_sin(index[:, None] * index[None, :], side)), BF16)
    low = np.arange(parts)
    tables = []
    for owner in range(groups):
        pair = cos_sin(low[:, None] * (owner * parts + low)[None, :], parts * groups)
        tables.append(np.stack(pair, 1))
    twiddle = jnp.asarray(np.stack(tables).reshape(-1), F32)

    chunks = steps * lanes
    block = (parts, 2, SUBLANE, LANE)
    by_way = (2, parts // SUB, 2, SUBLANE, LANE)
    vmem = pltpu.VMEM
    scratch = [
        vmem((2, parts, spokes, samples), BF16),
        vmem((1, spokes), I32),
        pltpu.SMEM((parts,), I32),
        vmem((segs, angles), I32),
        vmem((angles, segs, seg, seg), BF16),
        vmem((2, side, side), BF16),
        vmem((2, side, side), BF16),
        pltpu.SMEM(twiddle.shape, F32),
        vmem((across, 2 * side, 2 * hits), BF16),
        vmem((2 * side, 2 * side), BF16),
        vmem((angles, spokes), F32),
        vmem((segs, angles * SUBLANE, seg), F32),
        vmem((batches, 2 * share * (hits + SUBLANE), seg), F32),
        vmem((chunks, coils) + by_way, F32),
        vmem((chunks, groups) + by_way, F32),
        vmem((chunks,) + block, F32),
        vmem((chunks,) + block, F32),
    ]
    scratch += [vmem((chunks, coils >> (s + 1)) + by_way, F32) for s in range(bits)]
    dma = pltpu.SemaphoreType.DMA
    scratch += [dma((6,)), dma((batches,)), dma((CUTS,))]
    scratch += [dma((bits + 3,)), dma((steps + batches,)), dma((bits - 1, HALF_SLOTS))]
    scratch += [dma((batches * chunks,)), dma((INNER_SLOTS,))]
    anywhere = pl.BlockSpec(memory_space=pltpu.HBM)
    dims = (bits, groups, parts, rows, side, angles, segs, seg, spokes)
    return pl.pallas_call(
        functools.partial(kernel, dims),
        out_shape=pltpu.VMEM((2, parts, rows, side), F32),
        in_specs=[anywhere] * 8,
        out_specs=pl.BlockSpec(memory_space=pltpu.VMEM),
        scratch_shapes=scratch,
        compiler_params=pltpu.CompilerParams(
            collective_id=0, has_side_effects=True, vmem_limit_bytes=60 * 1024 * 1024
        ),
        name="reconstruct",
    )(
        kdata[:, :, 0],
        spoke_angle.reshape(1, -1),
        spoke_count,
        block_index.T,
        interp,
        sens_maps[:, 0],
        dft,
        twiddle,
    )


def solution(mesh):
    placed = (
        P(None, "kz", "coil", None, None),
        P(),
        P("kz"),
        P(),
        P(),
        P(None, "coil", None, None),
    )
    return jax.shard_map(
        per_device,
        mesh=mesh,
        in_specs=placed,
        out_specs=P(None, "kz", "coil", None),
        check_vma=False,
    )
```
